32 devices in a mesh: dp: 1 (over z), cp: 32 (over y, x, core).
Axes of the slice: x: 4, y: 4, z: 1, core: 2. Of those that a mesh axis runs over, the one named last changes fastest.
The devices are a block of a 4x4x8 slice.
Arguments:
- q_tok: bfloat16 [32768, 2, 128], P(('dp', 'cp'))
- k_tok: bfloat16 [32768, 128], P(('dp', 'cp'))
- v_tok: bfloat16 [32768, 128], P(('dp', 'cp'))
- fwd_out: bfloat16 [32768, 2, 128], P(('dp', 'cp'))
- d_out: bfloat16 [32768, 2, 128], P(('dp', 'cp'))
- lse_row: float32 [32768, 2], P(('dp', 'cp'))
Outputs:
- output 1: bfloat16 [32768, 2, 128], P(('dp', 'cp'))
- output 2: bfloat16 [32768, 128], P(('dp', 'cp'))
- output 3: bfloat16 [32768, 128], P(('dp', 'cp'))
All inputs are finite; a program needn't handle non-finite values.
Results may differ from the reference program's by a relative error of at most 0.001.
Values are sent between devices in bfloat16 or wider.
A program may use at most 768 MiB of HBM per device.

```python
import jax
import jax.numpy as jnp
from jax import lax

TOK_DEV = 1024
CP = 32
GQA = 2
HEAD = 128

SEQ = CP * TOK_DEV
Q_BLOCK = min(TOK_DEV, 128)
SOFTMAX_SCALE = HEAD ** -0.5
GRAD_GAIN = 0.25 * SEQ ** 0.5


def attention_forward(q_tok, k_tok, v_tok):
    k_full = k_tok.astype(jnp.float32)
    v_full = v_tok.astype(jnp.float32)
    columns = jnp.arange(SEQ)
    n_blocks = SEQ // Q_BLOCK

    def one_block(block_in):
        q_block, row_ids = block_in
        logits = jnp.einsum('rgd,cd->rgc', q_block.astype(jnp.float32), k_full) * SOFTMAX_SCALE
        allowed = columns[None, :] <= row_ids[:, None]
        logits = jnp.where(allowed[:, None, :], logits, -jnp.inf)
        lse_block = jax.nn.logsumexp(logits, axis=-1)
        prob_mat = jnp.exp(logits - lse_block[:, :, None])
        out_block = jnp.einsum('rgc,cd->rgd', prob_mat, v_full)
        return out_block.astype(jnp.bfloat16), lse_block

    out_blocks, lse_blocks = lax.map(one_block, (q_tok.reshape(n_blocks, Q_BLOCK, GQA, HEAD), columns.reshape(n_blocks, Q_BLOCK)))
    return out_blocks.reshape(SEQ, GQA, HEAD), lse_blocks.reshape(SEQ, GQA)


def setup_inputs(seed: int = 0, part: int = 0) -> dict:
    base_key = jax.random.fold_in(jax.random.key(seed), part)
    key_q, key_k, key_v, key_m, key_g = jax.random.split(base_key, 5)
    q_tok = jax.random.normal(key_q, (SEQ, GQA, HEAD), jnp.float32).astype(jnp.bfloat16)
    k_tok = jax.random.normal(key_k, (SEQ, HEAD), jnp.float32).astype(jnp.bfloat16)
    v_mean = jax.random.normal(key_m, (HEAD,), jnp.float32)
    v_tok = (v_mean[None, :] + jax.random.normal(key_v, (SEQ, HEAD), jnp.float32)).astype(jnp.bfloat16)
    d_out = (GRAD_GAIN * jax.random.normal(key_g, (SEQ, GQA, HEAD), jnp.float32)).astype(jnp.bfloat16)
    fwd_out, lse_row = attention_forward(q_tok, k_tok, v_tok)
    return {'q_tok': q_tok, 'k_tok': k_tok, 'v_tok': v_tok, 'fwd_out': fwd_out, 'd_out': d_out, 'lse_row': lse_row}


def reference(q_tok, k_tok, v_tok, fwd_out, d_out, lse_row):
    row_delta = jnp.sum(d_out.astype(jnp.float32) * fwd_out.astype(jnp.float32), axis=-1)
    k_full = k_tok.astype(jnp.float32)
    v_full = v_tok.astype(jnp.float32)
    columns = jnp.arange(SEQ)
    n_blocks = SEQ // Q_BLOCK

    def one_block(carry, block_in):
        dk_acc, dv_acc = carry
        q_block, do_block, lse_block, delta_block, row_ids = block_in
        q_wide = q_block.astype(jnp.float32)
        do_wide = do_block.astype(jnp.float32)
        logits = jnp.einsum('rgd,cd->rgc', q_wide, k_full) * SOFTMAX_SCALE
        allowed = columns[None, :] <= row_ids[:, None]
        prob_mat = jnp.exp(jnp.where(allowed[:, None, :], logits - lse_block[:, :, None], -jnp.inf))
        d_prob = jnp.einsum('rgd,cd->rgc', do_wide, v_full)
        d_score = prob_mat * (d_prob - delta_block[:, :, None])
        prob_low = prob_mat.astype(jnp.bfloat16).astype(jnp.float32)
        score_low = d_score.astype(jnp.bfloat16).astype(jnp.float32)
        dq_block = jnp.einsum('rgc,cd->rgd', score_low, k_full) * SOFTMAX_SCALE
        dk_acc = dk_acc + jnp.einsum('rgc,rgd->cd', score_low, q_wide)
        dv_acc = dv_acc + jnp.einsum('rgc,rgd->cd', prob_low, do_wide)
        return (dk_acc, dv_acc), dq_block.astype(jnp.bfloat16)

    acc_start = (jnp.zeros((SEQ, HEAD), jnp.float32), jnp.zeros((SEQ, HEAD), jnp.float32))
    block_inputs = (q_tok.reshape(n_blocks, Q_BLOCK, GQA, HEAD), d_out.reshape(n_blocks, Q_BLOCK, GQA, HEAD), lse_row.reshape(n_blocks, Q_BLOCK, GQA), row_delta.reshape(n_blocks, Q_BLOCK, GQA), columns.reshape(n_blocks, Q_BLOCK))
    (dk_acc, dv_acc), dq_blocks = lax.scan(one_block, acc_start, block_inputs)
    grad_q = dq_blocks.reshape(SEQ, GQA, HEAD)
    grad_k = (dk_acc * SOFTMAX_SCALE).astype(jnp.bfloat16)
    grad_v = dv_acc.astype(jnp.bfloat16)
    return (grad_q, grad_k, grad_v)
```

```python
import functools
import math

import jax
import jax.numpy as jnp
from jax import lax
from jax.experimental import pallas as pl
from jax.experimental.pallas import tpu as pltpu
from jax.sharding import PartitionSpec as P

MESH = pl.DeviceIdType.MESH
NT = (((1,), (1,)), ((), ()))
BF16, F32 = jnp.bfloat16, jnp.float32

ROWS = (
    [(q, dx, 0, 1) for q in (3, 2, 1) for dx in (1, 3, 2, 0)],
    [(2, 2, 1, 0), (2, 3, 1, 0), (3, 2, 1, 0), (3, 3, 1, 0)]
    + [(q, dx, 0, 1) for q in (3, 2) for dx in (1, 3, 2, 0)],
    [(2, 0, 1, 2), (2, 1, 1, 2), (3, 0, 1, 2), (3, 1, 1, 2)]
    + [(3, dx, 0, k) for dx in (1, 3, 2, 0) for k in (0, 1)],
    [(q, dx, 0, 2) for dx in (1, 3) for q in (3, 2, 1)]
    + [(q, dx, 0, 2) for q in (1, 2, 3) for dx in (2, 0)],
)
N_TASK = 12


def pack(rows, bits):
    return [sum(v << (bits * u) for u, v in enumerate(row)) for row in rows]


def last_use(row, key):
    return [int(all(key(e) != key(row[w]) for e in row[w + 1:])) for w in range(len(row))]


def first_use(row, key):
    return [int(all(key(e) != key(row[w]) for e in row[:w])) for w in range(len(row))]


T_Q = pack([[e[0] for e in r] for r in ROWS], 2)
T_X = pack([[e[1] for e in r] for r in ROWS], 2)
T_ABS = pack([[e[2] for e in r] for r in ROWS], 1)
T_KIND = pack([[e[3] for e in r] for r in ROWS], 2)
T_KVLAST = pack([last_use(r, lambda e: e[1:]) for r in ROWS], 1)
T_QLAST = pack([[f * int(e[0] != y) for f, e in zip(last_use(r, lambda e: e[0]), r)] for y, r in enumerate(ROWS)], 1)
T_QFIRST = pack([[f * int(e[0] != y) for f, e in zip(first_use(r, lambda e: e[0]), r)] for y, r in enumerate(ROWS)], 1)
T_TAKEN = pack([[f * int(e[3] == 2) for f, e in zip(first_use(r, lambda e: e[1:]), r)] for r in ROWS], 1)


def attn_grad_kernel(side, scale, q_hbm, do_hbm, st_hbm, k_hbm, v_hbm, gq_ref, gk_ref, gv_ref,
                     qb, dob, stb, qtb, dotb, kb, vb, dqa, dkv, dqr, par, ici, fin,
                     ld_sem, q_ss, q_rs, kv_s1, kv_s2, kv_s3, kv_s4, kv_rs,
                     par_ss, par_rs, ici_ss, ici_rs, dq_ss, dq_rs, fin_ss, fin_rs):
    rows2, head = qb.shape[1], qb.shape[2]
    tok = kb.shape[1]
    sub = tok // 4
    exp_scale = scale * math.log2(math.e)
    me = lax.axis_index('cp')
    c = lax.rem(me, 2)
    x = lax.rem(me // 2, side)
    y = me // (2 * side)
    partner = me + 1 - 2 * c
    own = 2 * x + c

    def dev(yy, xx, cc):
        return (yy * side + xx) * 2 + cc

    def wrap(v):
        return lax.rem(v, side)

    def copy(src, dst, ssem, rsem, device):
        return pltpu.make_async_remote_copy(src_ref=src, dst_ref=dst, send_sem=ssem, recv_sem=rsem,
                                            device_id={'cp': device}, device_id_type=MESH)

    def field(table, bits, u):
        word = jnp.where(y == 0, table[0], jnp.where(y == 1, table[1], jnp.where(y == 2, table[2], table[3])))
        return lax.rem(lax.shift_right_logical(word, bits * u), 1 << bits)

    def decode(u):
        kind = field(T_KIND, 2, u)
        xv = field(T_X, 2, u)
        xs = jnp.where(field(T_ABS, 1, u) == 1, xv, wrap(x + xv))
        taken = kind == 2
        slot = jnp.where(taken, 8 + xs, 2 * xs + kind)
        idx = jnp.where(taken, 4 + xs, xs)
        resp = jnp.where(taken, 0, kind)
        return slot, xs, idx, resp

    def feeds(src, dst):
        return jnp.logical_or(src < dst, jnp.logical_and(src == 3, jnp.logical_and(dst > 0, dst < 3)))

    def local_only(yy, xx, cc):
        low = jnp.logical_and(cc == 0, jnp.logical_or(yy == 0, jnp.logical_and(yy == 1, xx < 2)))
        return jnp.logical_or(yy == 3, low)

    gives = jnp.logical_and(c == 0, jnp.logical_or(y == 0, jnp.logical_and(y == 1, x < 2)))
    takes = jnp.logical_and(c == 0, jnp.logical_or(y == 3, jnp.logical_and(y == 2, x < 2)))
    mirror = dev(3 - y, x, c)

    loads = [pltpu.make_async_copy(src, dst, ld_sem.at[i]) for i, (src, dst) in enumerate((
        (k_hbm, kb.at[own]), (v_hbm, vb.at[own]), (q_hbm, qb.at[y]), (do_hbm, dob.at[y]), (st_hbm, stb.at[y])))]
    for load in loads:
        load.start()

    barrier = pltpu.get_barrier_semaphore()
    peers = [partner] + [dev(y, wrap(x + d), c) for d in (1, 2, 3)] + [dev(wrap(y + d), x, c) for d in (1, 2, 3)]
    for peer in peers:
        pl.semaphore_signal(barrier, inc=1, device_id={'cp': peer}, device_id_type=MESH)
    pl.semaphore_wait(barrier, len(peers))

    def kv_pair(slot, ssem, device):
        return (copy(kb.at[slot], kb.at[slot], ssem.at[0], kv_rs.at[slot, 0], device),
                copy(vb.at[slot], vb.at[slot], ssem.at[1], kv_rs.at[slot, 1], device))

    def start(pair):
        for p in pair:
            p.start()

    def kv_wait(slot):
        for p in kv_pair(slot, kv_s3, partner):
            p.wait_recv()

    def q_trio(row, dst_row):
        device = dev(dst_row, x, c)
        return tuple(copy(b.at[row], b.at[row], q_ss.at[dst_row, i], q_rs.at[row, i], device)
                     for i, b in enumerate((qb, dob, stb)))

    def par_copy(slot, idx):
        return copy(dkv.at[slot], par.at[idx], par_ss.at[idx], par_rs.at[idx], partner)

    def ici_copy(slot, xs, cls):
        return copy(dkv.at[slot], ici.at[4 * cls + x], ici_ss.at[4 * cls + xs], ici_rs.at[4 * cls + x], dev(y, xs, c))

    def ici_wait(cls, xs):
        copy(dkv.at[own], ici.at[4 * cls + xs], ici_ss.at[4 * cls + xs], ici_rs.at[4 * cls + xs], partner).wait_recv()

    def dq_copy(row):
        return copy(dqa.at[row], dqr.at[y], dq_ss.at[row], dq_rs.at[y], dev(row, x, c))

    def fin_copy():
        return copy(dkv.at[8 + x], fin, fin_ss, fin_rs, mirror)

    for load in loads[:2]:
        load.wait()
    start(kv_pair(own, kv_s1.at[0], partner))
    for d in (1, 3, 2):
        start(kv_pair(own, kv_s1.at[d], dev(y, wrap(x + d), c)))

    def give_copy():
        slot = 8 + x
        return (copy(kb.at[own], kb.at[slot], kv_s3.at[0], kv_rs.at[slot, 0], mirror),
                copy(vb.at[own], vb.at[slot], kv_s3.at[1], kv_rs.at[slot, 1], mirror))

    @pl.when(gives)
    def _():
        start(give_copy())

    for load in loads[2:]:
        load.wait()
    for d in (1, 3, 2):
        dst = wrap(y + d)

        @pl.when(feeds(dst, y))
        def _():
            start(q_trio(y, dst))

    def clear(ref, slots):
        def body(i, carry):
            ref[i] = jnp.zeros(ref.shape[1:], F32)
            return carry
        lax.fori_loop(0, slots, body, 0)

    clear(dkv, dkv.shape[0])
    clear(dqa, dqa.shape[0])

    def transpose_queries(row):
        for g in range(8):
            part = pl.ds(g * sub, sub)
            qtb[row, :, part] = qb[row, part, :].T
            dotb[row, :, part] = dob[row, part, :].T

    def piece(row, slot, start_row, width, u, masked):
        part = pl.ds(start_row, sub)
        k_t = kb[slot, :width, :]
        logits = lax.dot_general(qb[row, part, :], k_t, NT, preferred_element_type=F32)
        d_prob = lax.dot_general(dob[row, part, :], vb[slot, :width, :], NT, preferred_element_type=F32)
        stats = stb[row, :, part].T
        power = logits * exp_scale - stats[:, 0:1]
        if masked:
            r = lax.broadcasted_iota(jnp.int32, power.shape, 0) + u * sub
            power = jnp.where(lax.broadcasted_iota(jnp.int32, power.shape, 1) <= r, power, -1e30)
        prob = jnp.exp2(power)
        d_score = (prob * (d_prob - stats[:, 1:2])).astype(BF16)
        prob = prob.astype(BF16)
        dkv[slot, 1, :, :width] += jnp.dot(dotb[row, :, part], prob, preferred_element_type=F32)
        dkv[slot, 0, :, :width] += jnp.dot(qtb[row, :, part], d_score, preferred_element_type=F32)
        dqa[row, part, :] += jnp.dot(d_score, k_t, preferred_element_type=F32)

    def full_task(row, slot):
        def head_loop(g, carry):
            for u in range(4):
                piece(row, slot, pl.multiple_of(g * tok + u * sub, sub), tok, u, False)
            return carry
        lax.fori_loop(0, 2, head_loop, 0)

    def diag_task():
        def head_loop(g, carry):
            for u in range(4):
                piece(y, own, pl.multiple_of(g * tok + u * sub, sub), (u + 1) * sub, u, True)
            return carry
        lax.fori_loop(0, 2, head_loop, 0)

    def add_into(slot, other, oidx):
        def body(i, carry):
            part = pl.ds(pl.multiple_of(i * 32, 32), 32)
            for h in range(2):
                dkv[slot, h, part, :] += other[oidx, h, part, :]
            return carry
        lax.fori_loop(0, head // 32, body, 0)

    def reduce_chip(slot, xs, idx, cls):
        par_copy(slot, idx).wait_recv()
        add_into(slot, par, idx)

        @pl.when(xs != x)
        def _():
            ici_copy(slot, xs, cls).start()

    transpose_queries(y)
    diag_task()

    @pl.when(takes)
    def _():
        kv_wait(8 + x)
        start(kv_pair(8 + x, kv_s4.at[0], partner))
        for d in (1, 3, 2):
            start(kv_pair(8 + x, kv_s4.at[d], dev(y, wrap(x + d), c)))

    def after_diag(mine):
        for xs in range(4):
            cc = c if mine else 1 - c

            @pl.when(jnp.logical_and(local_only(y, xs, cc), xs <= x))
            def _():
                if mine:
                    reduce_chip(2 * xs + c, xs, xs, 0)
                else:
                    par_copy(2 * xs + 1 - c, xs).start()

    def step(t, carry):
        half = t // 2
        d = half + jnp.where(half == 2, 1, 0) - jnp.where(half == 3, 1, 0)
        x_d = wrap(x + d)
        mate = lax.rem(t, 2)
        c_d = jnp.where(mate == 0, c, 1 - c)
        u = jnp.maximum(t - 8, 0)
        first = t < 8
        slot_u, xs, idx, resp = decode(u)
        slot = jnp.where(first, 2 * x_d + c_d, slot_u)
        row = jnp.where(first, y, field(T_Q, 2, u))

        @pl.when(first)
        def _():
            kv_wait(slot)

            @pl.when(mate == 0)
            def _():
                start(kv_pair(slot, kv_s2.at[x_d], partner))

        later = jnp.logical_not(first)

        @pl.when(jnp.logical_and(later, field(T_QFIRST, 1, u) == 1))
        def _():
            for p in q_trio(row, row):
                p.wait_recv()
            transpose_queries(row)

        @pl.when(jnp.logical_and(later, field(T_TAKEN, 1, u) == 1))
        def _():
            @pl.when(jnp.logical_or(c == 1, xs != x))
            def _():
                kv_wait(slot)

            @pl.when(jnp.logical_and(c == 0, xs != x))
            def _():
                start(kv_pair(slot, kv_s2.at[4 + xs], partner))

        @pl.when(jnp.logical_or(later, 2 * x_d + c_d < own))
        def _():
            full_task(row, slot)

        @pl.when(t == 7)
        def _():
            after_diag(False)

        @pl.when(t == 9)
        def _():
            after_diag(True)

        @pl.when(jnp.logical_and(later, field(T_QLAST, 1, u) == 1))
        def _():
            dq_copy(row).start()

        done = field(T_KVLAST, 1, u) == 1

        @pl.when(jnp.logical_and(later, jnp.logical_and(done, c != resp)))
        def _():
            par_copy(slot, idx).start()

        before = jnp.maximum(u - 1, 0)
        slot_b, xs_b, idx_b, resp_b = decode(before)

        @pl.when(jnp.logical_and(u > 0, jnp.logical_and(field(T_KVLAST, 1, before) == 1, c == resp_b)))
        def _():
            reduce_chip(slot_b, xs_b, idx_b, idx_b // 4)
        return carry

    lax.fori_loop(1, 8 + N_TASK, step, 0)

    slot_b, xs_b, idx_b, resp_b = decode(jnp.int32(N_TASK - 1))

    @pl.when(c == resp_b)
    def _():
        reduce_chip(slot_b, xs_b, idx_b, idx_b // 4)

    @pl.when(takes)
    def _():
        for d in (1, 3, 2):
            ici_wait(1, wrap(x + d))
            add_into(8 + x, ici, 4 + wrap(x + d))
        fin_copy().start()

    for d in (1, 3, 2):
        xs = wrap(x + d)

        @pl.when(jnp.logical_or(jnp.logical_not(local_only(y, x, c)), xs > x))
        def _():
            ici_wait(0, xs)
            add_into(own, ici, xs)

    for d in (1, 3, 2):
        src = wrap(y + d)

        @pl.when(feeds(src, y))
        def _():
            copy(dqa.at[y], dqr.at[src], dq_ss.at[src], dq_rs.at[src], partner).wait_recv()

            def body(i, carry):
                part = pl.ds(pl.multiple_of(i * sub, sub), sub)
                dqa[y, part, :] += dqr[src, part, :]
                return carry
            lax.fori_loop(0, rows2 // sub, body, 0)

    @pl.when(gives)
    def _():
        fin_copy().wait_recv()

        def body(i, carry):
            part = pl.ds(pl.multiple_of(i * 32, 32), 32)
            for h in range(2):
                dkv[own, h, part, :] += fin[h, part, :]
            return carry
        lax.fori_loop(0, head // 32, body, 0)

    def out_q(i, carry):
        part = pl.ds(pl.multiple_of(i * sub, sub), sub)
        gq_ref[part, :] = (dqa[y, part, :] * scale).astype(BF16)
        return carry

    lax.fori_loop(0, rows2 // sub, out_q, 0)
    for g in range(4):
        part = pl.ds(g * sub, sub)
        gk_ref[part, :] = (dkv[own, 0, :, part] * scale).T.astype(BF16)
        gv_ref[part, :] = dkv[own, 1, :, part].T.astype(BF16)

    def sent(pair):
        for p in pair:
            p.wait_send()

    for d in range(4):
        sent(kv_pair(own, kv_s1.at[d], partner))
    for d in (1, 2, 3):
        sent(kv_pair(own, kv_s2.at[wrap(x + d)], partner))
        dst = wrap(y + d)

        @pl.when(feeds(dst, y))
        def _():
            sent(q_trio(y, dst))

        @pl.when(feeds(y, dst))
        def _():
            dq_copy(dst).wait_send()

    @pl.when(gives)
    def _():
        sent(give_copy())

    @pl.when(takes)
    def _():
        for d in range(4):
            sent(kv_pair(8 + x, kv_s4.at[d], partner))
        fin_copy().wait_send()

    for xs in range(4):
        has_taken = jnp.logical_or(y == 3, y == 2) if xs < 2 else y == 3

        @pl.when(jnp.logical_or(jnp.logical_not(local_only(y, xs, 1 - c)), xs <= x))
        def _():
            par_copy(2 * xs + 1 - c, xs).wait_send()

        @pl.when(jnp.logical_and(xs != x, jnp.logical_or(jnp.logical_not(local_only(y, xs, c)), xs < x)))
        def _():
            ici_copy(2 * xs + c, xs, 0).wait_send()

        @pl.when(jnp.logical_and(c == 1, has_taken))
        def _():
            par_copy(8 + xs, 4 + xs).wait_send()

        @pl.when(jnp.logical_and(jnp.logical_and(c == 0, xs != x), has_taken))
        def _():
            sent(kv_pair(8 + xs, kv_s2.at[4 + xs], partner))
            ici_copy(8 + xs, xs, 1).wait_send()


def solution(mesh):
    n_dev = mesh.shape['cp']
    side = math.isqrt(n_dev // 2)
    assert side * side * 2 == n_dev and side == len(ROWS)
    row_spec = P(('dp', 'cp'))

    def local_fn(q_tok, k_tok, v_tok, fwd_out, d_out, lse_row):
        tok, heads, head = q_tok.shape
        scale = head ** -0.5
        rows2 = tok * heads
        delta = jnp.sum(d_out.astype(F32) * fwd_out.astype(F32), axis=-1)
        stats = jnp.stack([lse_row * math.log2(math.e), delta]).transpose(0, 2, 1).reshape(2, rows2)
        stats = jnp.pad(stats, ((0, 6), (0, 0)))
        q_rows = q_tok.transpose(1, 0, 2).reshape(rows2, head)
        do_rows = d_out.transpose(1, 0, 2).reshape(rows2, head)
        hbm = pl.BlockSpec(memory_space=pl.ANY)
        vmem = pl.BlockSpec(memory_space=pltpu.VMEM)
        dma = pltpu.SemaphoreType.DMA
        gq, gk, gv = pl.pallas_call(
            functools.partial(attn_grad_kernel, side, scale),
            out_shape=[jax.ShapeDtypeStruct((rows2, head), BF16), jax.ShapeDtypeStruct((tok, head), BF16),
                       jax.ShapeDtypeStruct((tok, head), BF16)],
            in_specs=[hbm] * 5,
            out_specs=[vmem] * 3,
            scratch_shapes=[
                pltpu.VMEM((4, rows2, head), BF16), pltpu.VMEM((4, rows2, head), BF16), pltpu.VMEM((4, 8, rows2), F32),
                pltpu.VMEM((4, head, rows2), BF16), pltpu.VMEM((4, head, rows2), BF16),
                pltpu.VMEM((12, tok, head), BF16), pltpu.VMEM((12, tok, head), BF16),
                pltpu.VMEM((4, rows2, head), F32), pltpu.VMEM((12, 2, head, tok), F32), pltpu.VMEM((4, rows2, head), F32),
                pltpu.VMEM((8, 2, head, tok), F32), pltpu.VMEM((8, 2, head, tok), F32), pltpu.VMEM((2, head, tok), F32),
                dma((5,)), dma((4, 3)), dma((4, 3)), dma((4, 2)), dma((8, 2)), dma((2,)), dma((4, 2)), dma((12, 2)),
                dma((8,)), dma((8,)), dma((8,)), dma((8,)), dma((4,)), dma((4,)), dma, dma,
            ],
            compiler_params=pltpu.CompilerParams(collective_id=0, has_side_effects=True, vmem_limit_bytes=66 * 10 ** 6),
            name='attn_grad',
        )(q_rows, do_rows, stats, k_tok, v_tok)
        return gq.reshape(heads, tok, head).transpose(1, 0, 2), gk, gv

    return jax.shard_map(local_fn, mesh=mesh, in_specs=(row_spec,) * 6, out_specs=(row_spec,) * 3, check_vma=False)
```

```python
import functools
import math

import jax
import jax.numpy as jnp
from jax import lax
from jax.experimental import pallas as pl
from jax.experimental.pallas import tpu as pltpu
from jax.sharding import PartitionSpec as P

MESH = pl.DeviceIdType.MESH
NT = (((1,), (1,)), ((), ()))
BF16, F32 = jnp.bfloat16, jnp.float32

ROWS = (
    [(q, dx, 0, 1) for q in (3, 2, 1) for dx in (2, 1, 3, 0)],
    [(2, 2, 1, 0), (2, 3, 1, 0), (3, 2, 1, 0), (3, 3, 1, 0)]
    + [(q, dx, 0, 1) for q in (3, 2) for dx in (2, 1, 3, 0)],
    [(2, 0, 1, 2), (2, 1, 1, 2), (3, 0, 1, 2), (3, 1, 1, 2)]
    + [(3, dx, 0, k) for dx in (2, 1, 3, 0) for k in (0, 1)],
    [(q, dx, 0, 2) for dx in (2, 1) for q in (3, 2, 1)]
    + [(q, dx, 0, 2) for q in (1, 2, 3) for dx in (3, 0)],
)
N_TASK = 12


def pack(rows, bits):
    return [sum(v << (bits * u) for u, v in enumerate(row)) for row in rows]


def last_use(row, key):
    return [int(all(key(e) != key(row[w]) for e in row[w + 1:])) for w in range(len(row))]


def first_use(row, key):
    return [int(all(key(e) != key(row[w]) for e in row[:w])) for w in range(len(row))]


T_Q = pack([[e[0] for e in r] for r in ROWS], 2)
T_X = pack([[e[1] for e in r] for r in ROWS], 2)
T_ABS = pack([[e[2] for e in r] for r in ROWS], 1)
T_KIND = pack([[e[3] for e in r] for r in ROWS], 2)
T_KVLAST = pack([last_use(r, lambda e: e[1:]) for r in ROWS], 1)
T_QLAST = pack([[f * int(e[0] != y) for f, e in zip(last_use(r, lambda e: e[0]), r)] for y, r in enumerate(ROWS)], 1)
T_QFIRST = pack([[f * int(e[0] != y) for f, e in zip(first_use(r, lambda e: e[0]), r)] for y, r in enumerate(ROWS)], 1)
T_TAKEN = pack([[f * int(e[3] == 2) for f, e in zip(first_use(r, lambda e: e[1:]), r)] for r in ROWS], 1)


def attn_grad_kernel(side, scale, q_hbm, do_hbm, st_hbm, k_hbm, v_hbm, gq_ref, gk_ref, gv_ref,
                     qb, dob, stb, qtb, dotb, kb, vb, dqa, dkv, dqr, par, ici, half, fin,
                     ld_sem, q_ss, q_rs, kv_s1, kv_s2, kv_s3, kv_s4, kv_s5, kv_rs,
                     par_ss, par_rs, ici_ss, ici_rs, half_ss, half_rs, dq_ss, dq_rs, fin_ss, fin_rs):
    rows2, head = qb.shape[1], qb.shape[2]
    tok = kb.shape[1]
    sub = tok // 4
    exp_scale = scale * math.log2(math.e)
    me = lax.axis_index('cp')
    c = lax.rem(me, 2)
    x = lax.rem(me // 2, side)
    y = me // (2 * side)
    partner = me + 1 - 2 * c
    own = 2 * x + c

    def dev(yy, xx, cc):
        return (yy * side + xx) * 2 + cc

    def wrap(v):
        return lax.rem(v, side)

    def copy(src, dst, ssem, rsem, device):
        return pltpu.make_async_remote_copy(src_ref=src, dst_ref=dst, send_sem=ssem, recv_sem=rsem,
                                            device_id={'cp': device}, device_id_type=MESH)

    def field(table, bits, u):
        word = jnp.where(y == 0, table[0], jnp.where(y == 1, table[1], jnp.where(y == 2, table[2], table[3])))
        return lax.rem(lax.shift_right_logical(word, bits * u), 1 << bits)

    def decode(u):
        kind = field(T_KIND, 2, u)
        xv = field(T_X, 2, u)
        xs = jnp.where(field(T_ABS, 1, u) == 1, xv, wrap(x + xv))
        taken = kind == 2
        slot = jnp.where(taken, 8 + xs, 2 * xs + kind)
        idx = jnp.where(taken, 4 + xs, xs)
        resp = jnp.where(taken, 0, kind)
        return slot, xs, idx, resp

    def feeds(src, dst):
        return jnp.logical_or(src < dst, jnp.logical_and(src == 3, jnp.logical_and(dst > 0, dst < 3)))

    def local_only(yy, xx, cc):
        low = jnp.logical_and(cc == 0, jnp.logical_or(yy == 0, jnp.logical_and(yy == 1, xx < 2)))
        return jnp.logical_or(yy == 3, low)

    gives = jnp.logical_and(c == 0, jnp.logical_or(y == 0, jnp.logical_and(y == 1, x < 2)))
    takes = jnp.logical_and(c == 0, jnp.logical_or(y == 3, jnp.logical_and(y == 2, x < 2)))
    mirror = dev(3 - y, x, c)

    loads = [pltpu.make_async_copy(src, dst, ld_sem.at[i]) for i, (src, dst) in enumerate((
        (k_hbm, kb.at[own]), (v_hbm, vb.at[own]), (q_hbm, qb.at[y]), (do_hbm, dob.at[y]), (st_hbm, stb.at[y])))]
    for load in loads:
        load.start()

    barrier = pltpu.get_barrier_semaphore()
    peers = [partner] + [dev(y, wrap(x + d), c) for d in (1, 3)] + [dev(wrap(y + d), x, c) for d in (1, 3)]
    for peer in peers:
        pl.semaphore_signal(barrier, inc=1, device_id={'cp': peer}, device_id_type=MESH)
    pl.semaphore_wait(barrier, len(peers))

    def kv_pair(slot, ssem, device):
        return (copy(kb.at[slot], kb.at[slot], ssem.at[0], kv_rs.at[slot, 0], device),
                copy(vb.at[slot], vb.at[slot], ssem.at[1], kv_rs.at[slot, 1], device))

    def start(pair):
        for p in pair:
            p.start()

    def kv_wait(slot):
        for p in kv_pair(slot, kv_s3, partner):
            p.wait_recv()

    def q_trio(row, dst_row, relayed=0):
        device = dev(dst_row, x, c)
        return tuple(copy(b.at[row], b.at[row], q_ss.at[4 * relayed + dst_row, i], q_rs.at[row, i], device)
                     for i, b in enumerate((qb, dob, stb)))

    def q_wait(row):
        for p in q_trio(row, row):
            p.wait_recv()

    def kv_onward(slot, taken, toward):
        buf = kb if toward == 0 else vb
        return copy(buf.at[slot], buf.at[slot], kv_s5.at[2 * taken + toward], kv_rs.at[slot, toward],
                    dev(y, wrap(x + (1 if toward == 0 else 3)), c))

    def par_copy(slot, idx):
        return copy(dkv.at[slot], par.at[idx], par_ss.at[idx], par_rs.at[idx], partner)

    def ici_copy(slot, cls, side_in):
        device = dev(y, jnp.where(side_in == 0, wrap(x + 1), wrap(x + 3)), c)
        return copy(dkv.at[slot], ici.at[2 * cls + side_in], ici_ss.at[2 * cls + side_in],
                    ici_rs.at[2 * cls + side_in], device)

    def half_copy(slot, cls, h):
        return copy(dkv.at[slot, h], half.at[2 * cls + h], half_ss.at[2 * cls + h], half_rs.at[2 * cls + h],
                    dev(y, wrap(x + (1 if h == 0 else 3)), c))

    def dq_copy(row):
        up = row == y + 1
        dst = jnp.where(y == 3, jnp.where(row == 1, 0, 2), jnp.where(row == y + 3, 3, y + 1))
        place = jnp.where(up, 1, jnp.where(jnp.logical_or(row == y + 3, row == y - 1), 2, 0))
        return copy(dqa.at[row], dqr.at[place], dq_ss.at[row], dq_rs.at[place], dev(dst, x, c))

    def dq_take(row, place):
        copy(dqa.at[row], dqr.at[place], dq_ss.at[0], dq_rs.at[place], partner).wait_recv()

        def body(i, carry):
            part = pl.ds(pl.multiple_of(i * sub, sub), sub)
            dqa[row, part, :] += dqr[place, part, :]
            return carry
        lax.fori_loop(0, rows2 // sub, body, 0)

    def fin_copy():
        return copy(dkv.at[8 + x], fin, fin_ss, fin_rs, mirror)

    for load in loads[:2]:
        load.wait()
    start(kv_pair(own, kv_s1.at[0], partner))
    for d in (1, 3):
        start(kv_pair(own, kv_s1.at[d], dev(y, wrap(x + d), c)))

    def give_copy():
        slot = 8 + x
        return (copy(kb.at[own], kb.at[slot], kv_s3.at[0], kv_rs.at[slot, 0], mirror),
                copy(vb.at[own], vb.at[slot], kv_s3.at[1], kv_rs.at[slot, 1], mirror))

    @pl.when(gives)
    def _():
        start(give_copy())

    for load in loads[2:]:
        load.wait()
    for d in (1, 3):
        dst = wrap(y + d)

        @pl.when(feeds(dst, y))
        def _():
            start(q_trio(y, dst))

    def clear(ref, slots):
        def body(i, carry):
            ref[i] = jnp.zeros(ref.shape[1:], F32)
            return carry
        lax.fori_loop(0, slots, body, 0)

    clear(dkv, dkv.shape[0])
    clear(dqa, dqa.shape[0])

    def transpose_queries(row):
        for g in range(8):
            part = pl.ds(g * sub, sub)
            qtb[row, :, part] = qb[row, part, :].T
            dotb[row, :, part] = dob[row, part, :].T

    def piece(row, slot, start_row, width, u, masked):
        part = pl.ds(start_row, sub)
        k_t = kb[slot, :width, :]
        logits = lax.dot_general(qb[row, part, :], k_t, NT, preferred_element_type=F32)
        d_prob = lax.dot_general(dob[row, part, :], vb[slot, :width, :], NT, preferred_element_type=F32)
        stats = stb[row, :, part].T
        power = logits * exp_scale - stats[:, 0:1]
        if masked:
            r = (lax.broadcasted_iota(jnp.int32, power.shape, 0) + u * sub) // 2
            power = jnp.where(lax.broadcasted_iota(jnp.int32, power.shape, 1) <= r, power, -1e30)
        prob = jnp.exp2(power)
        d_score = (prob * (d_prob - stats[:, 1:2])).astype(BF16)
        prob = prob.astype(BF16)
        dkv[slot, 1, :, :width] += jnp.dot(dotb[row, :, part], prob, preferred_element_type=F32)
        dkv[slot, 0, :, :width] += jnp.dot(qtb[row, :, part], d_score, preferred_element_type=F32)
        dqa[row, part, :] += jnp.dot(d_score, k_t, preferred_element_type=F32)

    def full_task(row, slot):
        def half_loop(g, carry):
            for u in range(4):
                piece(row, slot, pl.multiple_of((4 * g + u) * sub, sub), tok, 0, False)
            return carry
        lax.fori_loop(0, 2, half_loop, 0)

    def diag_task():
        for u in range(8):
            piece(y, own, u * sub, (u // 2 + 1) * sub, u, True)

    def add_into(slot, h, other):
        def body(i, carry):
            part = pl.ds(pl.multiple_of(i * 32, 32), 32)
            dkv[slot, h, part, :] += other[part, :]
            return carry
        lax.fori_loop(0, head // 32, body, 0)

    def meets(xx, xs, cc):
        return jnp.logical_or(jnp.logical_not(local_only(y, xs, cc)), xx >= xs)

    def sum_chip(slot, xs, idx, cls):
        par_copy(slot, idx).wait_recv()
        for h in range(2):
            add_into(slot, h, par.at[idx, h])

        @pl.when(xs == wrap(x + 2))
        def _():
            for h in range(2):
                half_copy(slot, cls, h).start()

    def pass_on(slot, xs, cls, joined):
        for h in range(2):
            @pl.when(xs == wrap(x + (1 if h == 0 else 3)))
            def _():
                @pl.when(joined)
                def _():
                    half_copy(slot, cls, h).wait_recv()
                    add_into(slot, h, half.at[2 * cls + h])
                ici_copy(slot, cls, h).start()

    transpose_queries(y)
    diag_task()

    @pl.when(takes)
    def _():
        kv_wait(8 + x)
        start(kv_pair(8 + x, kv_s4.at[0], partner))
        for d in (1, 3):
            start(kv_pair(8 + x, kv_s4.at[d], dev(y, wrap(x + d), c)))

    def after_diag(stage):
        for xs in range(4):
            cc = 1 - c if stage == 0 else c
            alone = local_only(y, xs, cc)

            @pl.when(jnp.logical_and(alone, xs <= x if stage < 2 else jnp.logical_or(xs <= x, (xs + 2) % 4 >= xs)))
            def _():
                if stage == 0:
                    par_copy(2 * xs + 1 - c, xs).start()
                elif stage == 1:
                    sum_chip(2 * xs + c, xs, xs, 0)
                else:
                    pass_on(2 * xs + c, xs, 0, (xs + 2) % 4 >= xs)

    def taken_at(xs):
        return jnp.logical_or(y == 3, jnp.logical_and(y == 2, xs < 2))

    def step(t, carry):
        half = t // 2
        d = half + jnp.where(half == 2, 1, 0) - jnp.where(half == 3, 1, 0)
        x_d = wrap(x + d)
        mate = lax.rem(t, 2)
        c_d = jnp.where(mate == 0, c, 1 - c)
        u = jnp.maximum(t - 8, 0)
        first = t < 8
        slot_u, xs, idx, resp = decode(u)
        slot = jnp.where(first, 2 * x_d + c_d, slot_u)
        row = jnp.where(first, y, field(T_Q, 2, u))

        later = jnp.logical_not(first)

        @pl.when(jnp.logical_and(first, mate == 1))
        def _():
            kv_wait(slot)

        @pl.when(t == 2)
        def _():
            for toward, dd in ((0, 3), (1, 1)):
                near = 2 * wrap(x + dd) + c
                kv_wait(near)
                kv_onward(near, 0, toward).start()
                start(kv_pair(near, kv_s2.at[wrap(x + dd)], partner))

        @pl.when(t == 6)
        def _():
            kv_wait(slot)
            start(kv_pair(slot, kv_s2.at[x_d], partner))

        @pl.when(jnp.logical_and(t == 5, y == 0))
        def _():
            q_wait(3)
            start(q_trio(3, 1, 1))
            q_wait(1)
            start(q_trio(1, 3, 1))

        @pl.when(jnp.logical_and(t == 5, y == 1))
        def _():
            q_wait(2)
            start(q_trio(2, 0, 1))

        @pl.when(jnp.logical_and(t == 7, c == 0))
        def _():
            for toward, dd in ((0, 3), (1, 1)):
                near = wrap(x + dd)

                @pl.when(taken_at(near))
                def _():
                    kv_wait(8 + near)
                    kv_onward(8 + near, 1, toward).start()
                    start(kv_pair(8 + near, kv_s2.at[4 + near], partner))

        @pl.when(jnp.logical_and(later, field(T_QFIRST, 1, u) == 1))
        def _():
            relayed = jnp.logical_or(jnp.logical_and(y == 0, row != 2), jnp.logical_and(y == 1, row == 2))

            @pl.when(jnp.logical_not(relayed))
            def _():
                q_wait(row)
            transpose_queries(row)

        @pl.when(jnp.logical_and(later, field(T_TAKEN, 1, u) == 1))
        def _():
            far = xs == wrap(x + 2)

            @pl.when(jnp.logical_or(c == 1, far))
            def _():
                kv_wait(slot)

            @pl.when(jnp.logical_and(c == 0, far))
            def _():
                start(kv_pair(slot, kv_s2.at[4 + xs], partner))

        @pl.when(jnp.logical_or(later, 2 * x_d + c_d < own))
        def _():
            full_task(row, slot)

        for stage, when in ((0, 7), (1, 9), (2, 13)):
            @pl.when(t == when)
            def _():
                after_diag(stage)

        @pl.when(jnp.logical_and(later, field(T_QLAST, 1, u) == 1))
        def _():
            @pl.when(row == y + 1)
            def _():
                dq_take(row, 0)
            dq_copy(row).start()

        done = field(T_KVLAST, 1, u) == 1

        @pl.when(jnp.logical_and(later, jnp.logical_and(done, c != resp)))
        def _():
            par_copy(slot, idx).start()

        before = jnp.maximum(u - 1, 0)
        slot_b, xs_b, idx_b, resp_b = decode(before)

        @pl.when(jnp.logical_and(u > 0, jnp.logical_and(field(T_KVLAST, 1, before) == 1, c == resp_b)))
        def _():
            sum_chip(slot_b, xs_b, idx_b, idx_b // 4)
            pass_on(slot_b, xs_b, idx_b // 4, True)
        return carry

    lax.fori_loop(1, 8 + N_TASK, step, 0)

    slot_b, xs_b, idx_b, resp_b = decode(jnp.int32(N_TASK - 1))

    @pl.when(c == resp_b)
    def _():
        sum_chip(slot_b, xs_b, idx_b, idx_b // 4)
        pass_on(slot_b, xs_b, idx_b // 4, True)

    def from_side(slot, cls, side_in):
        ici_copy(slot, cls, side_in).wait_recv()
        for h in range(2):
            add_into(slot, h, ici.at[2 * cls + side_in, h])

    @pl.when(takes)
    def _():
        for side_in in range(2):
            from_side(8 + x, 1, side_in)
        fin_copy().start()

    for side_in in range(2):
        near = wrap(x + (3 if side_in == 0 else 1))

        @pl.when(jnp.logical_or(meets(near, x, c), meets(wrap(x + 2), x, c)))
        def _():
            from_side(own, 0, side_in)

    @pl.when(y >= 1)
    def _():
        dq_take(y, 1)

    @pl.when(y >= 2)
    def _():
        dq_take(y, 2)

    @pl.when(gives)
    def _():
        fin_copy().wait_recv()

        for h in range(2):
            add_into(own, h, fin.at[h])

    def out_q(i, carry):
        part = pl.ds(pl.multiple_of(i * sub, sub), sub)
        gq_ref[part, :] = (dqa[y, part, :] * scale).astype(BF16)
        return carry

    lax.fori_loop(0, rows2 // sub, out_q, 0)
    for g in range(4):
        part = pl.ds(g * sub, sub)
        gk_ref[part, :] = (dkv[own, 0, :, part] * scale).T.astype(BF16)
        gv_ref[part, :] = dkv[own, 1, :, part].T.astype(BF16)

    def sent(pair):
        for p in pair:
            p.wait_send()

    for d in (0, 1, 3):
        sent(kv_pair(own, kv_s1.at[d], partner))
    for h in range(2):
        kv_onward(own, 0, h).wait_send()
    for d in (1, 2, 3):
        sent(kv_pair(own, kv_s2.at[wrap(x + d)], partner))
    for d in (1, 3):
        dst = wrap(y + d)

        @pl.when(feeds(dst, y))
        def _():
            sent(q_trio(y, dst))

    @pl.when(y == 0)
    def _():
        sent(q_trio(3, 1, 1))
        sent(q_trio(1, 3, 1))

    @pl.when(y == 1)
    def _():
        sent(q_trio(2, 0, 1))

    for row in (1, 2, 3):
        @pl.when(jnp.logical_and(row != y, feeds(y, row)))
        def _():
            dq_copy(row).wait_send()

    @pl.when(gives)
    def _():
        sent(give_copy())

    @pl.when(takes)
    def _():
        for d in (0, 1, 3):
            sent(kv_pair(8 + x, kv_s4.at[d], partner))
        fin_copy().wait_send()

    for xs in range(4):
        @pl.when(meets(x, xs, 1 - c))
        def _():
            par_copy(2 * xs + 1 - c, xs).wait_send()

        @pl.when(jnp.logical_and(c == 1, taken_at(xs)))
        def _():
            par_copy(8 + xs, 4 + xs).wait_send()

        @pl.when(jnp.logical_and(jnp.logical_and(c == 0, xs != x), taken_at(xs)))
        def _():
            sent(kv_pair(8 + xs, kv_s2.at[4 + xs], partner))

    far = wrap(x + 2)
    for h in range(2):
        behind = wrap(x + (3 if h == 0 else 1))
        ahead = wrap(x + (1 if h == 0 else 3))

        @pl.when(jnp.logical_and(c == 0, taken_at(behind)))
        def _():
            kv_onward(8 + x, 1, h).wait_send()

        @pl.when(meets(x, far, c))
        def _():
            half_copy(own, 0, h).wait_send()

        @pl.when(jnp.logical_or(meets(x, ahead, c), meets(behind, ahead, c)))
        def _():
            ici_copy(own, 0, h).wait_send()

        @pl.when(jnp.logical_and(c == 0, taken_at(far)))
        def _():
            half_copy(own, 1, h).wait_send()

        @pl.when(jnp.logical_and(c == 0, taken_at(ahead)))
        def _():
            ici_copy(own, 1, h).wait_send()


def solution(mesh):
    n_dev = mesh.shape['cp']
    side = math.isqrt(n_dev // 2)
    assert side * side * 2 == n_dev and side == len(ROWS)
    row_spec = P(('dp', 'cp'))

    def local_fn(q_tok, k_tok, v_tok, fwd_out, d_out, lse_row):
        tok, heads, head = q_tok.shape
        scale = head ** -0.5
        rows2 = tok * heads
        delta = jnp.sum(d_out.astype(F32) * fwd_out.astype(F32), axis=-1)
        stats = jnp.stack([lse_row * math.log2(math.e), delta]).reshape(2, rows2)
        stats = jnp.pad(stats, ((0, 6), (0, 0)))
        q_rows = q_tok.reshape(rows2, head)
        do_rows = d_out.reshape(rows2, head)
        hbm = pl.BlockSpec(memory_space=pl.ANY)
        vmem = pl.BlockSpec(memory_space=pltpu.VMEM)
        dma = pltpu.SemaphoreType.DMA
        gq, gk, gv = pl.pallas_call(
            functools.partial(attn_grad_kernel, side, scale),
            out_shape=[jax.ShapeDtypeStruct((rows2, head), BF16), jax.ShapeDtypeStruct((tok, head), BF16),
                       jax.ShapeDtypeStruct((tok, head), BF16)],
            in_specs=[hbm] * 5,
            out_specs=[vmem] * 3,
            scratch_shapes=[
                pltpu.VMEM((4, rows2, head), BF16), pltpu.VMEM((4, rows2, head), BF16), pltpu.VMEM((4, 8, rows2), F32),
                pltpu.VMEM((4, head, rows2), BF16), pltpu.VMEM((4, head, rows2), BF16),
                pltpu.VMEM((12, tok, head), BF16), pltpu.VMEM((12, tok, head), BF16),
                pltpu.VMEM((4, rows2, head), F32), pltpu.VMEM((12, 2, head, tok), F32), pltpu.VMEM((3, rows2, head), F32),
                pltpu.VMEM((8, 2, head, tok), F32), pltpu.VMEM((4, 2, head, tok), F32), pltpu.VMEM((4, head, tok), F32),
                pltpu.VMEM((2, head, tok), F32),
                dma((5,)), dma((8, 3)), dma((4, 3)), dma((4, 2)), dma((8, 2)), dma((2,)), dma((4, 2)), dma((4,)), dma((12, 2)),
                dma((8,)), dma((8,)), dma((4,)), dma((4,)), dma((4,)), dma((4,)), dma((4,)), dma((3,)), dma, dma,
            ],
            compiler_params=pltpu.CompilerParams(collective_id=0, has_side_effects=True, vmem_limit_bytes=66 * 10 ** 6),
            name='attn_grad',
        )(q_rows, do_rows, stats, k_tok, v_tok)
        return gq.reshape(tok, heads, head), gk, gv

    return jax.shard_map(local_fn, mesh=mesh, in_specs=(row_spec,) * 6, out_specs=(row_spec,) * 3, check_vma=False)
```

```python
import functools
import math

import jax
import jax.numpy as jnp
from jax import lax
from jax.experimental import pallas as pl
from jax.experimental.pallas import tpu as pltpu
from jax.sharding import PartitionSpec as P

MESH = pl.DeviceIdType.MESH
NT = (((1,), (1,)), ((), ()))
BF16, F32 = jnp.bfloat16, jnp.float32

ROWS = (
    [(q, dx, 0, 1) for q in (3, 2, 1) for dx in (2, 1, 3, 0)],
    [(2, 2, 1, 0), (2, 3, 1, 0), (3, 2, 1, 0), (3, 3, 1, 0)]
    + [(q, dx, 0, 1) for q in (3, 2) for dx in (2, 1, 3, 0)],
    [(2, 0, 1, 2), (2, 1, 1, 2), (3, 0, 1, 2), (3, 1, 1, 2)]
    + [(3, dx, 0, k) for dx in (2, 1, 3, 0) for k in (0, 1)],
    [(q, dx, 0, 2) for dx in (2, 1) for q in (3, 2, 1)]
    + [(q, dx, 0, 2) for q in (1, 2, 3) for dx in (3, 0)],
)
N_TASK = 12
DELAY = 2


def pack(rows, bits):
    return [sum(v << (bits * u) for u, v in enumerate(row)) for row in rows]


def last_use(row, key):
    return [int(all(key(e) != key(row[w]) for e in row[w + 1:])) for w in range(len(row))]


def first_use(row, key):
    return [int(all(key(e) != key(row[w]) for e in row[:w])) for w in range(len(row))]


T_Q = pack([[e[0] for e in r] for r in ROWS], 2)
T_X = pack([[e[1] for e in r] for r in ROWS], 2)
T_ABS = pack([[e[2] for e in r] for r in ROWS], 1)
T_KIND = pack([[e[3] for e in r] for r in ROWS], 2)
T_KVLAST = pack([last_use(r, lambda e: e[1:]) for r in ROWS], 1)
T_QLAST = pack([[f * int(e[0] != y) for f, e in zip(last_use(r, lambda e: e[0]), r)] for y, r in enumerate(ROWS)], 1)
T_QFIRST = pack([[f * int(e[0] != y) for f, e in zip(first_use(r, lambda e: e[0]), r)] for y, r in enumerate(ROWS)], 1)
T_TAKEN = pack([[f * int(e[3] == 2) for f, e in zip(first_use(r, lambda e: e[1:]), r)] for r in ROWS], 1)


def attn_grad_kernel(side, scale, q_hbm, do_hbm, st_hbm, k_hbm, v_hbm, gq_ref, gk_ref, gv_ref,
                     qb, dob, stb, qtb, dotb, kb, vb, dqa, dkv, dqr, par, ici, half, fin,
                     ld_sem, q_ss, q_rs, kv_s1, kv_s2, kv_s3, kv_s4, kv_s5, kv_rs,
                     par_ss, par_rs, ici_ss, ici_rs, half_ss, half_rs, dq_ss, dq_rs, fin_ss, fin_rs):
    rows2, head = qb.shape[1], qb.shape[2]
    tok = kb.shape[1]
    sub = tok // 4
    exp_scale = scale * math.log2(math.e)
    me = lax.axis_index('cp')
    c = lax.rem(me, 2)
    x = lax.rem(me // 2, side)
    y = me // (2 * side)
    partner = me + 1 - 2 * c
    own = 2 * x + c

    def dev(yy, xx, cc):
        return (yy * side + xx) * 2 + cc

    def wrap(v):
        return lax.rem(v, side)

    def copy(src, dst, ssem, rsem, device):
        return pltpu.make_async_remote_copy(src_ref=src, dst_ref=dst, send_sem=ssem, recv_sem=rsem,
                                            device_id={'cp': device}, device_id_type=MESH)

    def field(table, bits, u):
        word = jnp.where(y == 0, table[0], jnp.where(y == 1, table[1], jnp.where(y == 2, table[2], table[3])))
        return lax.rem(lax.shift_right_logical(word, bits * u), 1 << bits)

    def decode(u):
        kind = field(T_KIND, 2, u)
        xv = field(T_X, 2, u)
        xs = jnp.where(field(T_ABS, 1, u) == 1, xv, wrap(x + xv))
        taken = kind == 2
        slot = jnp.where(taken, 8 + xs, 2 * xs + kind)
        idx = jnp.where(taken, 4 + xs, xs)
        resp = jnp.where(taken, 0, kind)
        return slot, xs, idx, resp

    def feeds(src, dst):
        return jnp.logical_or(src < dst, jnp.logical_and(src == 3, jnp.logical_and(dst > 0, dst < 3)))

    def local_only(yy, xx, cc):
        low = jnp.logical_and(cc == 0, jnp.logical_or(yy == 0, jnp.logical_and(yy == 1, xx < 2)))
        return jnp.logical_or(yy == 3, low)

    gives = jnp.logical_and(c == 0, jnp.logical_or(y == 0, jnp.logical_and(y == 1, x < 2)))
    takes = jnp.logical_and(c == 0, jnp.logical_or(y == 3, jnp.logical_and(y == 2, x < 2)))
    mirror = dev(3 - y, x, c)

    loads = [pltpu.make_async_copy(src, dst, ld_sem.at[i]) for i, (src, dst) in enumerate((
        (k_hbm, kb.at[own]), (v_hbm, vb.at[own]), (q_hbm, qb.at[y]), (do_hbm, dob.at[y]), (st_hbm, stb.at[y])))]
    for load in loads:
        load.start()

    barrier = pltpu.get_barrier_semaphore()
    peers = [partner] + [dev(y, wrap(x + d), c) for d in (1, 3)] + [dev(wrap(y + d), x, c) for d in (1, 3)]
    for peer in peers:
        pl.semaphore_signal(barrier, inc=1, device_id={'cp': peer}, device_id_type=MESH)
    pl.semaphore_wait(barrier, len(peers))

    def kv_pair(slot, ssem, device):
        return (copy(kb.at[slot], kb.at[slot], ssem.at[0], kv_rs.at[slot, 0], device),
                copy(vb.at[slot], vb.at[slot], ssem.at[1], kv_rs.at[slot, 1], device))

    def start(pair):
        for p in pair:
            p.start()

    def kv_wait(slot):
        for p in kv_pair(slot, kv_s3, partner):
            p.wait_recv()

    def q_trio(row, dst_row, relayed=0, parts=(0, 1, 2)):
        device = dev(dst_row, x, c)
        return tuple(copy(b.at[row], b.at[row], q_ss.at[4 * relayed + dst_row, i], q_rs.at[row, i], device)
                     for i, b in enumerate((qb, dob, stb)) if i in parts)

    def q_wait(row, parts=(0, 1, 2)):
        for p in q_trio(row, row, 0, parts):
            p.wait_recv()

    def kv_onward(slot, taken, toward):
        buf = kb if toward == 0 else vb
        return copy(buf.at[slot], buf.at[slot], kv_s5.at[2 * taken + toward], kv_rs.at[slot, toward],
                    dev(y, wrap(x + (1 if toward == 0 else 3)), c))

    def par_copy(slot, idx):
        return copy(dkv.at[slot], par.at[idx], par_ss.at[idx], par_rs.at[idx], partner)

    def ici_copy(slot, cls, side_in, h):
        device = dev(y, jnp.where(side_in == 0, wrap(x + 1), wrap(x + 3)), c)
        return copy(dkv.at[slot, h], ici.at[2 * cls + side_in, h], ici_ss.at[2 * cls + side_in, h],
                    ici_rs.at[2 * cls + side_in, h], device)

    def half_copy(slot, cls, h):
        return copy(dkv.at[slot, h], half.at[2 * cls + h], half_ss.at[2 * cls + h], half_rs.at[2 * cls + h],
                    dev(y, wrap(x + (1 if h == 0 else 3)), c))

    def dq_copy(row, h):
        up = row == y + 1
        dst = jnp.where(y == 3, jnp.where(row == 1, 0, 2), jnp.where(row == y + 3, 3, y + 1))
        place = jnp.where(up, 1, jnp.where(jnp.logical_or(row == y + 3, row == y - 1), 2, 0))
        part = pl.ds(h * tok, tok)
        return copy(dqa.at[row, part], dqr.at[place, part], dq_ss.at[row, h], dq_rs.at[place, h], dev(dst, x, c))

    def dq_take(row, place, h):
        half_rows = pl.ds(h * tok, tok)
        copy(dqa.at[row, half_rows], dqr.at[place, half_rows], dq_ss.at[0, h], dq_rs.at[place, h], partner).wait_recv()

        def body(i, carry):
            part = pl.ds(pl.multiple_of(h * tok + i * sub, sub), sub)
            dqa[row, part, :] += dqr[place, part, :]
            return carry
        lax.fori_loop(0, tok // sub, body, 0)

    def fin_copy(h):
        return copy(dkv.at[8 + x, h], fin.at[h], fin_ss.at[h], fin_rs.at[h], mirror)

    for load in loads[:2]:
        load.wait()
    start(kv_pair(own, kv_s1.at[0], partner))
    for d in (1, 3):
        start(kv_pair(own, kv_s1.at[d], dev(y, wrap(x + d), c)))

    def give_copy():
        slot = 8 + x
        return (copy(kb.at[own], kb.at[slot], kv_s3.at[0], kv_rs.at[slot, 0], mirror),
                copy(vb.at[own], vb.at[slot], kv_s3.at[1], kv_rs.at[slot, 1], mirror))

    @pl.when(gives)
    def _():
        start(give_copy())

    for load in loads[2:]:
        load.wait()
    for d in (1, 3):
        dst = wrap(y + d)

        @pl.when(feeds(dst, y))
        def _():
            start(q_trio(y, dst))

    def clear(ref, slots):
        def body(i, carry):
            ref[i] = jnp.zeros(ref.shape[1:], F32)
            return carry
        lax.fori_loop(0, slots, body, 0)

    clear(dkv, dkv.shape[0])
    clear(dqa, dqa.shape[0])

    def transpose_queries(row):
        for g in range(8):
            part = pl.ds(g * sub, sub)
            qtb[row, :, part] = qb[row, part, :].T
            dotb[row, :, part] = dob[row, part, :].T

    def piece(row, slot, start_row, width, u, masked):
        part = pl.ds(start_row, sub)
        k_t = kb[slot, :width, :]
        logits = lax.dot_general(qb[row, part, :], k_t, NT, preferred_element_type=F32)
        d_prob = lax.dot_general(dob[row, part, :], vb[slot, :width, :], NT, preferred_element_type=F32)
        stats = stb[row, :, part].T
        power = logits * exp_scale - stats[:, 0:1]
        if masked:
            r = (lax.broadcasted_iota(jnp.int32, power.shape, 0) + u * sub) // 2
            power = jnp.where(lax.broadcasted_iota(jnp.int32, power.shape, 1) <= r, power, -1e30)
        prob = jnp.exp2(power)
        d_score = (prob * (d_prob - stats[:, 1:2])).astype(BF16)
        prob = prob.astype(BF16)
        dkv[slot, 1, :, :width] += jnp.dot(dotb[row, :, part], prob, preferred_element_type=F32)
        dkv[slot, 0, :, :width] += jnp.dot(qtb[row, :, part], d_score, preferred_element_type=F32)
        dqa[row, part, :] += jnp.dot(d_score, k_t, preferred_element_type=F32)

    def full_task(row, slot):
        def half_loop(g, carry):
            for u in range(4):
                piece(row, slot, pl.multiple_of((4 * g + u) * sub, sub), tok, 0, False)
            return carry
        lax.fori_loop(0, 2, half_loop, 0)

    def diag_task():
        for u in range(8):
            piece(y, own, u * sub, (u // 2 + 1) * sub, u, True)

    def add_into(slot, h, other):
        def body(i, carry):
            part = pl.ds(pl.multiple_of(i * 32, 32), 32)
            dkv[slot, h, part, :] += other[part, :]
            return carry
        lax.fori_loop(0, head // 32, body, 0)

    def meets(xx, xs, cc):
        return jnp.logical_or(jnp.logical_not(local_only(y, xs, cc)), xx >= xs)

    def sum_chip(slot, xs, idx, cls):
        par_copy(slot, idx).wait_recv()
        for h in range(2):
            add_into(slot, h, par.at[idx, h])

        @pl.when(xs == wrap(x + 2))
        def _():
            for h in range(2):
                half_copy(slot, cls, h).start()

    def pass_on(slot, xs, cls, joined):
        for h in range(2):
            @pl.when(xs == wrap(x + (1 if h == 0 else 3)))
            def _():
                @pl.when(joined)
                def _():
                    half_copy(slot, cls, h).wait_recv()
                    add_into(slot, h, half.at[2 * cls + h])
                for part in range(2):
                    ici_copy(slot, cls, h, part).start()

    transpose_queries(y)
    diag_task()

    @pl.when(takes)
    def _():
        kv_wait(8 + x)
        start(kv_pair(8 + x, kv_s4.at[0], partner))
        for d in (1, 3):
            start(kv_pair(8 + x, kv_s4.at[d], dev(y, wrap(x + d), c)))

    def after_diag(stage):
        for xs in range(4):
            cc = 1 - c if stage == 0 else c
            alone = local_only(y, xs, cc)

            @pl.when(jnp.logical_and(alone, xs <= x if stage < 2 else jnp.logical_or(xs <= x, (xs + 2) % 4 >= xs)))
            def _():
                if stage == 0:
                    par_copy(2 * xs + 1 - c, xs).start()
                elif stage == 1:
                    sum_chip(2 * xs + c, xs, xs, 0)
                else:
                    pass_on(2 * xs + c, xs, 0, (xs + 2) % 4 >= xs)

    def taken_at(xs):
        return jnp.logical_or(y == 3, jnp.logical_and(y == 2, xs < 2))

    def step(t, carry):
        half = t // 2
        d = half + jnp.where(half == 2, 1, 0) - jnp.where(half == 3, 1, 0)
        x_d = wrap(x + d)
        mate = lax.rem(t, 2)
        c_d = jnp.where(mate == 0, c, 1 - c)
        u = jnp.maximum(t - 8, 0)
        first = t < 8
        slot_u, xs, idx, resp = decode(u)
        slot = jnp.where(first, 2 * x_d + c_d, slot_u)
        row = jnp.where(first, y, field(T_Q, 2, u))

        later = jnp.logical_not(first)

        @pl.when(jnp.logical_and(first, mate == 1))
        def _():
            kv_wait(slot)

        @pl.when(t == 2)
        def _():
            for toward, dd in ((0, 3), (1, 1)):
                near = 2 * wrap(x + dd) + c
                kv_wait(near)
                kv_onward(near, 0, toward).start()
                start(kv_pair(near, kv_s2.at[wrap(x + dd)], partner))

        @pl.when(t == 6)
        def _():
            kv_wait(slot)
            start(kv_pair(slot, kv_s2.at[x_d], partner))

        for when, parts in ((3, (0,)), (5, (1, 2))):
            @pl.when(jnp.logical_and(t == when, y == 0))
            def _():
                q_wait(3, parts)
                start(q_trio(3, 1, 1, parts))
                q_wait(1, parts)
                start(q_trio(1, 3, 1, parts))

            @pl.when(jnp.logical_and(t == when, y == 1))
            def _():
                q_wait(2, parts)
                start(q_trio(2, 0, 1, parts))

        @pl.when(jnp.logical_and(t == 7, c == 0))
        def _():
            for toward, dd in ((0, 3), (1, 1)):
                near = wrap(x + dd)

                @pl.when(taken_at(near))
                def _():
                    kv_wait(8 + near)
                    kv_onward(8 + near, 1, toward).start()
                    start(kv_pair(8 + near, kv_s2.at[4 + near], partner))

        @pl.when(jnp.logical_and(later, field(T_QFIRST, 1, u) == 1))
        def _():
            relayed = jnp.logical_or(jnp.logical_and(y == 0, row != 2), jnp.logical_and(y == 1, row == 2))

            @pl.when(jnp.logical_not(relayed))
            def _():
                q_wait(row)
            transpose_queries(row)

        @pl.when(jnp.logical_and(later, field(T_TAKEN, 1, u) == 1))
        def _():
            far = xs == wrap(x + 2)

            @pl.when(jnp.logical_or(c == 1, far))
            def _():
                kv_wait(slot)

            @pl.when(jnp.logical_and(c == 0, far))
            def _():
                start(kv_pair(slot, kv_s2.at[4 + xs], partner))

        @pl.when(jnp.logical_or(later, 2 * x_d + c_d < own))
        def _():
            full_task(row, slot)

        for stage, when in ((0, 12), (1, 14), (2, 16)):
            @pl.when(t == when)
            def _():
                after_diag(stage)

        @pl.when(jnp.logical_and(later, field(T_QLAST, 1, u) == 1))
        def _():
            for h in range(2):
                @pl.when(row == y + 1)
                def _():
                    dq_take(row, 0, h)
                dq_copy(row, h).start()

        done = field(T_KVLAST, 1, u) == 1

        @pl.when(jnp.logical_and(later, jnp.logical_and(done, c != resp)))
        def _():
            par_copy(slot, idx).start()

        def finished(back, action):
            before = jnp.maximum(u - back, 0)
            slot_b, xs_b, idx_b, resp_b = decode(before)

            @pl.when(jnp.logical_and(u >= back, jnp.logical_and(field(T_KVLAST, 1, before) == 1, c == resp_b)))
            def _():
                action(slot_b, xs_b, idx_b)

        finished(1, lambda slot_b, xs_b, idx_b: sum_chip(slot_b, xs_b, idx_b, idx_b // 4))
        finished(1 + DELAY, lambda slot_b, xs_b, idx_b: pass_on(slot_b, xs_b, idx_b // 4, True))
        return carry

    lax.fori_loop(1, 8 + N_TASK, step, 0)

    for u_b in range(N_TASK - 1 - DELAY, N_TASK):
        slot_b, xs_b, idx_b, resp_b = decode(jnp.int32(u_b))

        @pl.when(jnp.logical_and(field(T_KVLAST, 1, u_b) == 1, c == resp_b))
        def _():
            if u_b == N_TASK - 1:
                sum_chip(slot_b, xs_b, idx_b, idx_b // 4)
            pass_on(slot_b, xs_b, idx_b // 4, True)

    def from_side(slot, cls, side_in, h):
        ici_copy(slot, cls, side_in, h).wait_recv()
        add_into(slot, h, ici.at[2 * cls + side_in, h])

    @pl.when(takes)
    def _():
        for h in range(2):
            for side_in in range(2):
                from_side(8 + x, 1, side_in, h)
            fin_copy(h).start()

    for side_in in range(2):
        near = wrap(x + (3 if side_in == 0 else 1))

        @pl.when(jnp.logical_or(meets(near, x, c), meets(wrap(x + 2), x, c)))
        def _():
            for h in range(2):
                from_side(own, 0, side_in, h)

    for h in range(2):
        @pl.when(y >= 1)
        def _():
            dq_take(y, 1, h)

        @pl.when(y >= 2)
        def _():
            dq_take(y, 2, h)

    @pl.when(gives)
    def _():
        for h in range(2):
            fin_copy(h).wait_recv()
            add_into(own, h, fin.at[h])

    def out_q(i, carry):
        part = pl.ds(pl.multiple_of(i * sub, sub), sub)
        gq_ref[part, :] = (dqa[y, part, :] * scale).astype(BF16)
        return carry

    lax.fori_loop(0, rows2 // sub, out_q, 0)
    for g in range(4):
        part = pl.ds(g * sub, sub)
        gk_ref[part, :] = (dkv[own, 0, :, part] * scale).T.astype(BF16)
        gv_ref[part, :] = dkv[own, 1, :, part].T.astype(BF16)

    def sent(pair):
        for p in pair:
            p.wait_send()

    for d in (0, 1, 3):
        sent(kv_pair(own, kv_s1.at[d], partner))
    for h in range(2):
        kv_onward(own, 0, h).wait_send()
    for d in (1, 2, 3):
        sent(kv_pair(own, kv_s2.at[wrap(x + d)], partner))
    for d in (1, 3):
        dst = wrap(y + d)

        @pl.when(feeds(dst, y))
        def _():
            sent(q_trio(y, dst))

    @pl.when(y == 0)
    def _():
        sent(q_trio(3, 1, 1))
        sent(q_trio(1, 3, 1))

    @pl.when(y == 1)
    def _():
        sent(q_trio(2, 0, 1))

    for row in (1, 2, 3):
        @pl.when(jnp.logical_and(row != y, feeds(y, row)))
        def _():
            for h in range(2):
                dq_copy(row, h).wait_send()

    @pl.when(gives)
    def _():
        sent(give_copy())

    @pl.when(takes)
    def _():
        for d in (0, 1, 3):
            sent(kv_pair(8 + x, kv_s4.at[d], partner))
        for h in range(2):
            fin_copy(h).wait_send()

    for xs in range(4):
        @pl.when(meets(x, xs, 1 - c))
        def _():
            par_copy(2 * xs + 1 - c, xs).wait_send()

        @pl.when(jnp.logical_and(c == 1, taken_at(xs)))
        def _():
            par_copy(8 + xs, 4 + xs).wait_send()

        @pl.when(jnp.logical_and(jnp.logical_and(c == 0, xs != x), taken_at(xs)))
        def _():
            sent(kv_pair(8 + xs, kv_s2.at[4 + xs], partner))

    far = wrap(x + 2)
    for h in range(2):
        behind = wrap(x + (3 if h == 0 else 1))
        ahead = wrap(x + (1 if h == 0 else 3))

        @pl.when(jnp.logical_and(c == 0, taken_at(behind)))
        def _():
            kv_onward(8 + x, 1, h).wait_send()

        @pl.when(meets(x, far, c))
        def _():
            half_copy(own, 0, h).wait_send()

        @pl.when(jnp.logical_or(meets(x, ahead, c), meets(behind, ahead, c)))
        def _():
            for part in range(2):
                ici_copy(own, 0, h, part).wait_send()

        @pl.when(jnp.logical_and(c == 0, taken_at(far)))
        def _():
            half_copy(own, 1, h).wait_send()

        @pl.when(jnp.logical_and(c == 0, taken_at(ahead)))
        def _():
            for part in range(2):
                ici_copy(own, 1, h, part).wait_send()


def solution(mesh):
    n_dev = mesh.shape['cp']
    side = math.isqrt(n_dev // 2)
    assert side * side * 2 == n_dev and side == len(ROWS)
    row_spec = P(('dp', 'cp'))

    def local_fn(q_tok, k_tok, v_tok, fwd_out, d_out, lse_row):
        tok, heads, head = q_tok.shape
        scale = head ** -0.5
        rows2 = tok * heads
        delta = jnp.sum(d_out.astype(F32) * fwd_out.astype(F32), axis=-1)
        stats = jnp.stack([lse_row * math.log2(math.e), delta]).reshape(2, rows2)
        stats = jnp.pad(stats, ((0, 6), (0, 0)))
        q_rows = q_tok.reshape(rows2, head)
        do_rows = d_out.reshape(rows2, head)
        hbm = pl.BlockSpec(memory_space=pl.ANY)
        vmem = pl.BlockSpec(memory_space=pltpu.VMEM)
        dma = pltpu.SemaphoreType.DMA
        gq, gk, gv = pl.pallas_call(
            functools.partial(attn_grad_kernel, side, scale),
            out_shape=[jax.ShapeDtypeStruct((rows2, head), BF16), jax.ShapeDtypeStruct((tok, head), BF16),
                       jax.ShapeDtypeStruct((tok, head), BF16)],
            in_specs=[hbm] * 5,
            out_specs=[vmem] * 3,
            scratch_shapes=[
                pltpu.VMEM((4, rows2, head), BF16), pltpu.VMEM((4, rows2, head), BF16), pltpu.VMEM((4, 8, rows2), F32),
                pltpu.VMEM((4, head, rows2), BF16), pltpu.VMEM((4, head, rows2), BF16),
                pltpu.VMEM((12, tok, head), BF16), pltpu.VMEM((12, tok, head), BF16),
                pltpu.VMEM((4, rows2, head), F32), pltpu.VMEM((12, 2, head, tok), F32), pltpu.VMEM((3, rows2, head), F32),
                pltpu.VMEM((8, 2, head, tok), F32), pltpu.VMEM((4, 2, head, tok), F32), pltpu.VMEM((4, head, tok), F32),
                pltpu.VMEM((2, head, tok), F32),
                dma((5,)), dma((8, 3)), dma((4, 3)), dma((4, 2)), dma((8, 2)), dma((2,)), dma((4, 2)), dma((4,)), dma((12, 2)),
                dma((8,)), dma((8,)), dma((4, 2)), dma((4, 2)), dma((4,)), dma((4,)), dma((4, 2)), dma((3, 2)), dma((2,)), dma((2,)),
            ],
            compiler_params=pltpu.CompilerParams(collective_id=0, has_side_effects=True, vmem_limit_bytes=66 * 10 ** 6),
            name='attn_grad',
        )(q_rows, do_rows, stats, k_tok, v_tok)
        return gq.reshape(tok, heads, head), gk, gv

    return jax.shard_map(local_fn, mesh=mesh, in_specs=(row_spec,) * 6, out_specs=(row_spec,) * 3, check_vma=False)
```

```python
import functools
import math

import jax
import jax.numpy as jnp
from jax import lax
from jax.experimental import pallas as pl
from jax.experimental.pallas import tpu as pltpu
from jax.sharding import PartitionSpec as P

MESH = pl.DeviceIdType.MESH
NT = (((1,), (1,)), ((), ()))
BF16, F32 = jnp.bfloat16, jnp.float32

ROWS = (
    [(q, dx, 0, 1) for q in (3, 2, 1) for dx in (2, 1, 3, 0)],
    [(2, 2, 1, 0), (2, 3, 1, 0), (3, 2, 1, 0), (3, 3, 1, 0)]
    + [(q, dx, 0, 1) for q in (3, 2) for dx in (2, 1, 3, 0)],
    [(2, 0, 1, 2), (2, 1, 1, 2), (3, 0, 1, 2), (3, 1, 1, 2)]
    + [(3, dx, 0, k) for dx in (2, 1, 3, 0) for k in (0, 1)],
    [(q, dx, 0, 2) for dx in (2, 1) for q in (3, 2, 1)]
    + [(q, dx, 0, 2) for q in (1, 2, 3) for dx in (3, 0)],
)
N_TASK = 12
DELAY = 2


def pack(rows, bits):
    return [sum(v << (bits * u) for u, v in enumerate(row)) for row in rows]


def last_use(row, key):
    return [int(all(key(e) != key(row[w]) for e in row[w + 1:])) for w in range(len(row))]


def first_use(row, key):
    return [int(all(key(e) != key(row[w]) for e in row[:w])) for w in range(len(row))]


T_Q = pack([[e[0] for e in r] for r in ROWS], 2)
T_X = pack([[e[1] for e in r] for r in ROWS], 2)
T_ABS = pack([[e[2] for e in r] for r in ROWS], 1)
T_KIND = pack([[e[3] for e in r] for r in ROWS], 2)
T_KVLAST = pack([last_use(r, lambda e: e[1:]) for r in ROWS], 1)
T_QLAST = pack([[f * int(e[0] != y) for f, e in zip(last_use(r, lambda e: e[0]), r)] for y, r in enumerate(ROWS)], 1)
T_QFIRST = pack([[f * int(e[0] != y) for f, e in zip(first_use(r, lambda e: e[0]), r)] for y, r in enumerate(ROWS)], 1)
T_TAKEN = pack([[f * int(e[3] == 2) for f, e in zip(first_use(r, lambda e: e[1:]), r)] for r in ROWS], 1)


def attn_grad_kernel(side, scale, q_hbm, do_hbm, o_hbm, lse_hbm, k_hbm, v_hbm, gq_ref, gk_ref, gv_ref,
                     qb, dob, stb, ob, lseb, qtb, dotb, kb, vb, dqa, dkv, dqr, par, ici, half, fin,
                     ld_sem, q_ss, q_rs, kv_s1, kv_s2, kv_s3, kv_s4, kv_s5, kv_rs,
                     par_ss, par_rs, ici_ss, ici_rs, half_ss, half_rs, dq_ss, dq_rs, fin_ss, fin_rs):
    rows2, head = qb.shape[1], qb.shape[2]
    tok = kb.shape[1]
    sub = tok // 4
    exp_scale = scale * math.log2(math.e)
    me = lax.axis_index('cp')
    c = lax.rem(me, 2)
    x = lax.rem(me // 2, side)
    y = me // (2 * side)
    partner = me + 1 - 2 * c
    own = 2 * x + c

    def dev(yy, xx, cc):
        return (yy * side + xx) * 2 + cc

    def wrap(v):
        return lax.rem(v, side)

    def copy(src, dst, ssem, rsem, device):
        return pltpu.make_async_remote_copy(src_ref=src, dst_ref=dst, send_sem=ssem, recv_sem=rsem,
                                            device_id={'cp': device}, device_id_type=MESH)

    def field(table, bits, u):
        word = jnp.where(y == 0, table[0], jnp.where(y == 1, table[1], jnp.where(y == 2, table[2], table[3])))
        return lax.rem(lax.shift_right_logical(word, bits * u), 1 << bits)

    def decode(u):
        kind = field(T_KIND, 2, u)
        xv = field(T_X, 2, u)
        xs = jnp.where(field(T_ABS, 1, u) == 1, xv, wrap(x + xv))
        taken = kind == 2
        slot = jnp.where(taken, 8 + xs, 2 * xs + kind)
        idx = jnp.where(taken, 4 + xs, xs)
        resp = jnp.where(taken, 0, kind)
        return slot, xs, idx, resp

    def feeds(src, dst):
        return jnp.logical_or(src < dst, jnp.logical_and(src == 3, jnp.logical_and(dst > 0, dst < 3)))

    def local_only(yy, xx, cc):
        low = jnp.logical_and(cc == 0, jnp.logical_or(yy == 0, jnp.logical_and(yy == 1, xx < 2)))
        return jnp.logical_or(yy == 3, low)

    gives = jnp.logical_and(c == 0, jnp.logical_or(y == 0, jnp.logical_and(y == 1, x < 2)))
    takes = jnp.logical_and(c == 0, jnp.logical_or(y == 3, jnp.logical_and(y == 2, x < 2)))
    mirror = dev(3 - y, x, c)

    loads = [pltpu.make_async_copy(src, dst, ld_sem.at[i]) for i, (src, dst) in enumerate((
        (k_hbm, kb.at[own]), (v_hbm, vb.at[own]), (q_hbm, qb.at[y]), (do_hbm, dob.at[y]), (o_hbm, ob), (lse_hbm, lseb)))]
    for load in loads:
        load.start()

    barrier = pltpu.get_barrier_semaphore()
    peers = [partner] + [dev(y, wrap(x + d), c) for d in (1, 3)] + [dev(wrap(y + d), x, c) for d in (1, 3)]
    for peer in peers:
        pl.semaphore_signal(barrier, inc=1, device_id={'cp': peer}, device_id_type=MESH)
    pl.semaphore_wait(barrier, len(peers))

    def kv_pair(slot, ssem, device):
        return (copy(kb.at[slot], kb.at[slot], ssem.at[0], kv_rs.at[slot, 0], device),
                copy(vb.at[slot], vb.at[slot], ssem.at[1], kv_rs.at[slot, 1], device))

    def start(pair):
        for p in pair:
            p.start()

    def kv_wait(slot):
        for p in kv_pair(slot, kv_s3, partner):
            p.wait_recv()

    def q_trio(row, dst_row, relayed=0, parts=(0, 1, 2)):
        device = dev(dst_row, x, c)
        return tuple(copy(b.at[row], b.at[row], q_ss.at[4 * relayed + dst_row, i], q_rs.at[row, i], device)
                     for i, b in enumerate((qb, dob, stb)) if i in parts)

    def q_wait(row, parts=(0, 1, 2)):
        for p in q_trio(row, row, 0, parts):
            p.wait_recv()

    def kv_onward(slot, taken, toward):
        buf = kb if toward == 0 else vb
        return copy(buf.at[slot], buf.at[slot], kv_s5.at[2 * taken + toward], kv_rs.at[slot, toward],
                    dev(y, wrap(x + (1 if toward == 0 else 3)), c))

    def par_copy(slot, idx):
        return copy(dkv.at[slot], par.at[idx], par_ss.at[idx], par_rs.at[idx], partner)

    def ici_copy(slot, cls, side_in, h):
        device = dev(y, jnp.where(side_in == 0, wrap(x + 1), wrap(x + 3)), c)
        return copy(dkv.at[slot, h], ici.at[2 * cls + side_in, h], ici_ss.at[2 * cls + side_in, h],
                    ici_rs.at[2 * cls + side_in, h], device)

    def half_copy(slot, cls, h):
        return copy(dkv.at[slot, h], half.at[2 * cls + h], half_ss.at[2 * cls + h], half_rs.at[2 * cls + h],
                    dev(y, wrap(x + (1 if h == 0 else 3)), c))

    def dq_copy(row, h):
        up = row == y + 1
        dst = jnp.where(y == 3, jnp.where(row == 1, 0, 2), jnp.where(row == y + 3, 3, y + 1))
        place = jnp.where(up, 1, jnp.where(jnp.logical_or(row == y + 3, row == y - 1), 2, 0))
        part = pl.ds(h * tok, tok)
        return copy(dqa.at[row, part], dqr.at[place, part], dq_ss.at[row, h], dq_rs.at[place, h], dev(dst, x, c))

    def dq_take(row, place, h):
        half_rows = pl.ds(h * tok, tok)
        copy(dqa.at[row, half_rows], dqr.at[place, half_rows], dq_ss.at[0, h], dq_rs.at[place, h], partner).wait_recv()

        def body(i, carry):
            part = pl.ds(pl.multiple_of(h * tok + i * sub, sub), sub)
            dqa[row, part, :] += dqr[place, part, :]
            return carry
        lax.fori_loop(0, tok // sub, body, 0)

    def fin_copy(h):
        return copy(dkv.at[8 + x, h], fin.at[h], fin_ss.at[h], fin_rs.at[h], mirror)

    for load in loads[:2]:
        load.wait()
    start(kv_pair(own, kv_s1.at[0], partner))
    for d in (1, 3):
        start(kv_pair(own, kv_s1.at[d], dev(y, wrap(x + d), c)))

    def give_copy():
        slot = 8 + x
        return (copy(kb.at[own], kb.at[slot], kv_s3.at[0], kv_rs.at[slot, 0], mirror),
                copy(vb.at[own], vb.at[slot], kv_s3.at[1], kv_rs.at[slot, 1], mirror))

    @pl.when(gives)
    def _():
        start(give_copy())

    for load in loads[2:]:
        load.wait()

    def feed(parts):
        for d in (1, 3):
            dst = wrap(y + d)

            @pl.when(feeds(dst, y))
            def _():
                start(q_trio(y, dst, 0, parts))

    feed((0, 1))

    def clear(ref, slots):
        def body(i, carry):
            ref[i] = jnp.zeros(ref.shape[1:], F32)
            return carry
        lax.fori_loop(0, slots, body, 0)

    def row_stats():
        stb[y] = jnp.zeros(stb.shape[1:], F32)
        pair = (sub // 2, sub)
        spread = (lax.broadcasted_iota(jnp.int32, pair, 1) // 2 == lax.broadcasted_iota(jnp.int32, pair, 0)).astype(F32)
        even = lax.broadcasted_iota(jnp.int32, (1, sub), 1) % 2 == 0
        for p in range(rows2 // sub):
            part = pl.ds(p * sub, sub)
            lse = lseb[:, pl.ds(p * sub // 2, sub // 2)] * math.log2(math.e)
            lse = jnp.dot(lse, spread, precision=lax.Precision.HIGHEST, preferred_element_type=F32)
            stb[y, 0:1, part] = jnp.where(even, lse[0:1], lse[1:2])
            prod = dob[y, part, :].astype(F32) * ob[part, :].astype(F32)
            stb[y, 1:2, part] = jnp.sum(prod.T, axis=0, keepdims=True)

    row_stats()
    clear(dkv, dkv.shape[0])
    feed((2,))
    clear(dqa, dqa.shape[0])

    def transpose_queries(row):
        for g in range(8):
            part = pl.ds(g * sub, sub)
            qtb[row, :, part] = qb[row, part, :].T
            dotb[row, :, part] = dob[row, part, :].T

    def piece(row, slot, start_row, width, u, masked):
        part = pl.ds(start_row, sub)
        k_t = kb[slot, :width, :]
        logits = lax.dot_general(qb[row, part, :], k_t, NT, preferred_element_type=F32)
        d_prob = lax.dot_general(dob[row, part, :], vb[slot, :width, :], NT, preferred_element_type=F32)
        stats = stb[row, :, part].T
        power = logits * exp_scale - stats[:, 0:1]
        if masked:
            r = (lax.broadcasted_iota(jnp.int32, power.shape, 0) + u * sub) // 2
            power = jnp.where(lax.broadcasted_iota(jnp.int32, power.shape, 1) <= r, power, -1e30)
        prob = jnp.exp2(power)
        d_score = (prob * (d_prob - stats[:, 1:2])).astype(BF16)
        prob = prob.astype(BF16)
        dkv[slot, 1, :, :width] += jnp.dot(dotb[row, :, part], prob, preferred_element_type=F32)
        dkv[slot, 0, :, :width] += jnp.dot(qtb[row, :, part], d_score, preferred_element_type=F32)
        dqa[row, part, :] += jnp.dot(d_score, k_t, preferred_element_type=F32)

    def full_task(row, slot):
        for u in range(rows2 // sub):
            piece(row, slot, u * sub, tok, 0, False)

    def diag_task():
        for u in range(8):
            piece(y, own, u * sub, (u // 2 + 1) * sub, u, True)

    def add_into(slot, h, other):
        def body(i, carry):
            part = pl.ds(pl.multiple_of(i * 32, 32), 32)
            dkv[slot, h, part, :] += other[part, :]
            return carry
        lax.fori_loop(0, head // 32, body, 0)

    def meets(xx, xs, cc):
        return jnp.logical_or(jnp.logical_not(local_only(y, xs, cc)), xx >= xs)

    def sum_chip(slot, xs, idx, cls):
        par_copy(slot, idx).wait_recv()
        for h in range(2):
            add_into(slot, h, par.at[idx, h])

        @pl.when(xs == wrap(x + 2))
        def _():
            for h in range(2):
                half_copy(slot, cls, h).start()

    def pass_on(slot, xs, cls, joined):
        for h in range(2):
            @pl.when(xs == wrap(x + (1 if h == 0 else 3)))
            def _():
                @pl.when(joined)
                def _():
                    half_copy(slot, cls, h).wait_recv()
                    add_into(slot, h, half.at[2 * cls + h])
                for part in range(2):
                    ici_copy(slot, cls, h, part).start()

    transpose_queries(y)
    diag_task()

    @pl.when(takes)
    def _():
        kv_wait(8 + x)
        start(kv_pair(8 + x, kv_s4.at[0], partner))
        for d in (1, 3):
            start(kv_pair(8 + x, kv_s4.at[d], dev(y, wrap(x + d), c)))

    def after_diag(stage):
        for xs in range(4):
            cc = 1 - c if stage == 0 else c
            alone = local_only(y, xs, cc)

            @pl.when(jnp.logical_and(alone, xs <= x if stage < 2 else jnp.logical_or(xs <= x, (xs + 2) % 4 >= xs)))
            def _():
                if stage == 0:
                    par_copy(2 * xs + 1 - c, xs).start()
                elif stage == 1:
                    sum_chip(2 * xs + c, xs, xs, 0)
                else:
                    pass_on(2 * xs + c, xs, 0, (xs + 2) % 4 >= xs)

    def taken_at(xs):
        return jnp.logical_or(y == 3, jnp.logical_and(y == 2, xs < 2))

    def step(t, carry):
        half = t // 2
        d = half + jnp.where(half == 2, 1, 0) - jnp.where(half == 3, 1, 0)
        x_d = wrap(x + d)
        mate = lax.rem(t, 2)
        c_d = jnp.where(mate == 0, c, 1 - c)
        u = jnp.maximum(t - 8, 0)
        first = t < 8
        slot_u, xs, idx, resp = decode(u)
        slot = jnp.where(first, 2 * x_d + c_d, slot_u)
        row = jnp.where(first, y, field(T_Q, 2, u))

        later = jnp.logical_not(first)

        @pl.when(jnp.logical_and(first, mate == 1))
        def _():
            kv_wait(slot)

        @pl.when(t == 2)
        def _():
            for toward, dd in ((0, 3), (1, 1)):
                near = 2 * wrap(x + dd) + c
                kv_wait(near)
                kv_onward(near, 0, toward).start()
                start(kv_pair(near, kv_s2.at[wrap(x + dd)], partner))

        @pl.when(t == 6)
        def _():
            kv_wait(slot)
            start(kv_pair(slot, kv_s2.at[x_d], partner))

        for when, parts in ((3, (0,)), (5, (1, 2))):
            @pl.when(jnp.logical_and(t == when, y == 0))
            def _():
                q_wait(3, parts)
                start(q_trio(3, 1, 1, parts))
                q_wait(1, parts)
                start(q_trio(1, 3, 1, parts))

            @pl.when(jnp.logical_and(t == when, y == 1))
            def _():
                q_wait(2, parts)
                start(q_trio(2, 0, 1, parts))

        @pl.when(jnp.logical_and(t == 7, c == 0))
        def _():
            for toward, dd in ((0, 3), (1, 1)):
                near = wrap(x + dd)

                @pl.when(taken_at(near))
                def _():
                    kv_wait(8 + near)
                    kv_onward(8 + near, 1, toward).start()
                    start(kv_pair(8 + near, kv_s2.at[4 + near], partner))

        @pl.when(jnp.logical_and(later, field(T_QFIRST, 1, u) == 1))
        def _():
            relayed = jnp.logical_or(jnp.logical_and(y == 0, row != 2), jnp.logical_and(y == 1, row == 2))

            @pl.when(jnp.logical_not(relayed))
            def _():
                q_wait(row)
            transpose_queries(row)

        @pl.when(jnp.logical_and(later, field(T_TAKEN, 1, u) == 1))
        def _():
            far = xs == wrap(x + 2)

            @pl.when(jnp.logical_or(c == 1, far))
            def _():
                kv_wait(slot)

            @pl.when(jnp.logical_and(c == 0, far))
            def _():
                start(kv_pair(slot, kv_s2.at[4 + xs], partner))

        @pl.when(jnp.logical_or(later, 2 * x_d + c_d < own))
        def _():
            full_task(row, slot)

        for stage, when in ((0, 12), (1, 14), (2, 16)):
            @pl.when(t == when)
            def _():
                after_diag(stage)

        @pl.when(jnp.logical_and(later, field(T_QLAST, 1, u) == 1))
        def _():
            for h in range(2):
                @pl.when(row == y + 1)
                def _():
                    dq_take(row, 0, h)
                dq_copy(row, h).start()

        done = field(T_KVLAST, 1, u) == 1

        @pl.when(jnp.logical_and(later, jnp.logical_and(done, c != resp)))
        def _():
            par_copy(slot, idx).start()

        def finished(back, action):
            before = jnp.maximum(u - back, 0)
            slot_b, xs_b, idx_b, resp_b = decode(before)

            @pl.when(jnp.logical_and(u >= back, jnp.logical_and(field(T_KVLAST, 1, before) == 1, c == resp_b)))
            def _():
                action(slot_b, xs_b, idx_b)

        finished(1, lambda slot_b, xs_b, idx_b: sum_chip(slot_b, xs_b, idx_b, idx_b // 4))
        finished(1 + DELAY, lambda slot_b, xs_b, idx_b: pass_on(slot_b, xs_b, idx_b // 4, True))
        return carry

    lax.fori_loop(1, 8 + N_TASK, step, 0)

    for u_b in range(N_TASK - 1 - DELAY, N_TASK):
        slot_b, xs_b, idx_b, resp_b = decode(jnp.int32(u_b))

        @pl.when(jnp.logical_and(field(T_KVLAST, 1, u_b) == 1, c == resp_b))
        def _():
            if u_b == N_TASK - 1:
                sum_chip(slot_b, xs_b, idx_b, idx_b // 4)
            pass_on(slot_b, xs_b, idx_b // 4, True)

    def from_side(slot, cls, side_in, h):
        ici_copy(slot, cls, side_in, h).wait_recv()
        add_into(slot, h, ici.at[2 * cls + side_in, h])

    @pl.when(takes)
    def _():
        for h in range(2):
            for side_in in range(2):
                from_side(8 + x, 1, side_in, h)
            fin_copy(h).start()

    for side_in in range(2):
        near = wrap(x + (3 if side_in == 0 else 1))

        @pl.when(jnp.logical_or(meets(near, x, c), meets(wrap(x + 2), x, c)))
        def _():
            for h in range(2):
                from_side(own, 0, side_in, h)

    for h in range(2):
        @pl.when(y >= 1)
        def _():
            dq_take(y, 1, h)

        @pl.when(y >= 2)
        def _():
            dq_take(y, 2, h)

    @pl.when(gives)
    def _():
        for h in range(2):
            fin_copy(h).wait_recv()
            add_into(own, h, fin.at[h])

    def out_q(i, carry):
        part = pl.ds(pl.multiple_of(i * sub, sub), sub)
        gq_ref[part, :] = (dqa[y, part, :] * scale).astype(BF16)
        return carry

    lax.fori_loop(0, rows2 // sub, out_q, 0)
    for g in range(4):
        part = pl.ds(g * sub, sub)
        gk_ref[part, :] = (dkv[own, 0, :, part] * scale).T.astype(BF16)
        gv_ref[part, :] = dkv[own, 1, :, part].T.astype(BF16)

    def sent(pair):
        for p in pair:
            p.wait_send()

    for d in (0, 1, 3):
        sent(kv_pair(own, kv_s1.at[d], partner))
    for h in range(2):
        kv_onward(own, 0, h).wait_send()
    for d in (1, 2, 3):
        sent(kv_pair(own, kv_s2.at[wrap(x + d)], partner))
    for d in (1, 3):
        dst = wrap(y + d)

        @pl.when(feeds(dst, y))
        def _():
            sent(q_trio(y, dst))

    @pl.when(y == 0)
    def _():
        sent(q_trio(3, 1, 1))
        sent(q_trio(1, 3, 1))

    @pl.when(y == 1)
    def _():
        sent(q_trio(2, 0, 1))

    for row in (1, 2, 3):
        @pl.when(jnp.logical_and(row != y, feeds(y, row)))
        def _():
            for h in range(2):
                dq_copy(row, h).wait_send()

    @pl.when(gives)
    def _():
        sent(give_copy())

    @pl.when(takes)
    def _():
        for d in (0, 1, 3):
            sent(kv_pair(8 + x, kv_s4.at[d], partner))
        for h in range(2):
            fin_copy(h).wait_send()

    for xs in range(4):
        @pl.when(meets(x, xs, 1 - c))
        def _():
            par_copy(2 * xs + 1 - c, xs).wait_send()

        @pl.when(jnp.logical_and(c == 1, taken_at(xs)))
        def _():
            par_copy(8 + xs, 4 + xs).wait_send()

        @pl.when(jnp.logical_and(jnp.logical_and(c == 0, xs != x), taken_at(xs)))
        def _():
            sent(kv_pair(8 + xs, kv_s2.at[4 + xs], partner))

    far = wrap(x + 2)
    for h in range(2):
        behind = wrap(x + (3 if h == 0 else 1))
        ahead = wrap(x + (1 if h == 0 else 3))

        @pl.when(jnp.logical_and(c == 0, taken_at(behind)))
        def _():
            kv_onward(8 + x, 1, h).wait_send()

        @pl.when(meets(x, far, c))
        def _():
            half_copy(own, 0, h).wait_send()

        @pl.when(jnp.logical_or(meets(x, ahead, c), meets(behind, ahead, c)))
        def _():
            for part in range(2):
                ici_copy(own, 0, h, part).wait_send()

        @pl.when(jnp.logical_and(c == 0, taken_at(far)))
        def _():
            half_copy(own, 1, h).wait_send()

        @pl.when(jnp.logical_and(c == 0, taken_at(ahead)))
        def _():
            for part in range(2):
                ici_copy(own, 1, h, part).wait_send()


def solution(mesh):
    n_dev = mesh.shape['cp']
    side = math.isqrt(n_dev // 2)
    assert side * side * 2 == n_dev and side == len(ROWS)
    row_spec = P(('dp', 'cp'))

    def local_fn(q_tok, k_tok, v_tok, fwd_out, d_out, lse_row):
        tok, heads, head = q_tok.shape
        scale = head ** -0.5
        rows2 = tok * heads
        q_rows = q_tok.reshape(rows2, head)
        do_rows = d_out.reshape(rows2, head)
        o_rows = fwd_out.reshape(rows2, head)
        hbm = pl.BlockSpec(memory_space=pl.ANY)
        vmem = pl.BlockSpec(memory_space=pltpu.VMEM)
        slots = 3 * side
        line, grid = pltpu.SemaphoreType.DMA((8,)), pltpu.SemaphoreType.DMA((slots, 3))
        rows_low = pltpu.VMEM((side, rows2, head), BF16)
        cols_low = pltpu.VMEM((side, head, rows2), BF16)
        keys = pltpu.VMEM((slots, tok, head), BF16)

        def sums(n):
            return pltpu.VMEM((n, 2, head, tok), F32)

        gq, gk, gv = pl.pallas_call(
            functools.partial(attn_grad_kernel, side, scale),
            out_shape=[jax.ShapeDtypeStruct((rows2, head), BF16), jax.ShapeDtypeStruct((tok, head), BF16),
                       jax.ShapeDtypeStruct((tok, head), BF16)],
            in_specs=[hbm] * 6,
            out_specs=[vmem] * 3,
            scratch_shapes=[
                rows_low, rows_low, pltpu.VMEM((side, 8, rows2), F32), pltpu.VMEM((rows2, head), BF16),
                pltpu.VMEM((heads, tok), F32), cols_low, cols_low, keys, keys, pltpu.VMEM((side, rows2, head), F32),
                sums(slots), pltpu.VMEM((3, rows2, head), F32), sums(8), sums(side), pltpu.VMEM((side, head, tok), F32),
                pltpu.VMEM((2, head, tok), F32), line, grid, grid, grid, grid, line, grid, line, grid,
                line, line, grid, grid, line, line, grid, grid, line, line,
            ],
            compiler_params=pltpu.CompilerParams(collective_id=0, has_side_effects=True, vmem_limit_bytes=66 * 10 ** 6),
            name='attn_grad',
        )(q_rows, do_rows, o_rows, lse_row.T, k_tok, v_tok)
        return gq.reshape(tok, heads, head), gk, gv

    return jax.shard_map(local_fn, mesh=mesh, in_specs=(row_spec,) * 6, out_specs=(row_spec,) * 3, check_vma=False)
```

```python
import functools
import math

import jax
import jax.numpy as jnp
from jax import lax
from jax.experimental import pallas as pl
from jax.experimental.pallas import tpu as pltpu
from jax.sharding import PartitionSpec as P

MESH = pl.DeviceIdType.MESH
NT = (((1,), (1,)), ((), ()))
BF16, F32 = jnp.bfloat16, jnp.float32

ROWS = (
    [(q, dx, 0, 1) for q in (3, 2, 1) for dx in (2, 1, 3, 0)],
    [(2, 2, 1, 0), (2, 3, 1, 0), (3, 2, 1, 0), (3, 3, 1, 0)]
    + [(q, dx, 0, 1) for q in (3, 2) for dx in (2, 1, 3, 0)],
    [(2, 0, 1, 2), (2, 1, 1, 2), (3, 0, 1, 2), (3, 1, 1, 2)]
    + [(3, dx, 0, k) for dx in (2, 1, 3, 0) for k in (0, 1)],
    [(q, dx, 0, 2) for dx in (2, 1) for q in (3, 2, 1)]
    + [(q, dx, 0, 2) for q in (1, 2, 3) for dx in (3, 0)],
)
N_TASK = 12
SPLIT = 2
WHOLE = N_TASK - SPLIT
N_STEP = WHOLE + 2 * SPLIT
DELAY = 2


def pack(rows, bits):
    return [sum(v << (bits * u) for u, v in enumerate(row)) for row in rows]


def last_use(row, key):
    return [int(all(key(e) != key(row[w]) for e in row[w + 1:])) for w in range(len(row))]


def first_use(row, key):
    return [int(all(key(e) != key(row[w]) for e in row[:w])) for w in range(len(row))]


T_Q = pack([[e[0] for e in r] for r in ROWS], 2)
T_X = pack([[e[1] for e in r] for r in ROWS], 2)
T_ABS = pack([[e[2] for e in r] for r in ROWS], 1)
T_KIND = pack([[e[3] for e in r] for r in ROWS], 2)
T_KVLAST = pack([last_use(r, lambda e: e[1:]) for r in ROWS], 1)
T_QLAST = pack([[f * int(e[0] != y) for f, e in zip(last_use(r, lambda e: e[0]), r)] for y, r in enumerate(ROWS)], 1)
T_QFIRST = pack([[f * int(e[0] != y) for f, e in zip(first_use(r, lambda e: e[0]), r)] for y, r in enumerate(ROWS)], 1)
T_TAKEN = pack([[f * int(e[3] == 2) for f, e in zip(first_use(r, lambda e: e[1:]), r)] for r in ROWS], 1)


def attn_grad_kernel(side, scale, q_hbm, do_hbm, o_hbm, lse_hbm, k_hbm, v_hbm, gq_ref, gk_ref, gv_ref,
                     qb, dob, stb, ob, lseb, qtb, dotb, kb, vb, dqa, dkv, dqr, par, ici, half, fin,
                     ld_sem, q_ss, q_rs, kv_s1, kv_s2, kv_s3, kv_s4, kv_s5, kv_rs,
                     par_ss, par_rs, ici_ss, ici_rs, half_ss, half_rs, dq_ss, dq_rs, fin_ss, fin_rs):
    rows2, head = qb.shape[1], qb.shape[2]
    tok = kb.shape[1]
    sub = tok // 4
    exp_scale = scale * math.log2(math.e)
    me = lax.axis_index('cp')
    c = lax.rem(me, 2)
    x = lax.rem(me // 2, side)
    y = me // (2 * side)
    partner = me + 1 - 2 * c
    own = 2 * x + c

    def dev(yy, xx, cc):
        return (yy * side + xx) * 2 + cc

    def wrap(v):
        return lax.rem(v, side)

    def copy(src, dst, ssem, rsem, device):
        return pltpu.make_async_remote_copy(src_ref=src, dst_ref=dst, send_sem=ssem, recv_sem=rsem,
                                            device_id={'cp': device}, device_id_type=MESH)

    def field(table, bits, u):
        word = jnp.where(y == 0, table[0], jnp.where(y == 1, table[1], jnp.where(y == 2, table[2], table[3])))
        return lax.rem(lax.shift_right_logical(word, bits * u), 1 << bits)

    def decode(u):
        kind = field(T_KIND, 2, u)
        xv = field(T_X, 2, u)
        xs = jnp.where(field(T_ABS, 1, u) == 1, xv, wrap(x + xv))
        taken = kind == 2
        slot = jnp.where(taken, 8 + xs, 2 * xs + kind)
        idx = jnp.where(taken, 4 + xs, xs)
        resp = jnp.where(taken, 0, kind)
        return slot, xs, idx, resp

    def unit(v):
        w = v - WHOLE
        by_half = y < 3
        which = jnp.where(by_half, lax.rem(w, 2), w // 2)
        part = jnp.where(by_half, w // 2, lax.rem(w, 2))
        return jnp.where(w < 0, v, WHOLE + which), jnp.maximum(part, 0), jnp.logical_or(w < 0, part == 1)

    def feeds(src, dst):
        return jnp.logical_or(src < dst, jnp.logical_and(src == 3, jnp.logical_and(dst > 0, dst < 3)))

    def local_only(yy, xx, cc):
        low = jnp.logical_and(cc == 0, jnp.logical_or(yy == 0, jnp.logical_and(yy == 1, xx < 2)))
        return jnp.logical_or(yy == 3, low)

    gives = jnp.logical_and(c == 0, jnp.logical_or(y == 0, jnp.logical_and(y == 1, x < 2)))
    takes = jnp.logical_and(c == 0, jnp.logical_or(y == 3, jnp.logical_and(y == 2, x < 2)))
    mirror = dev(3 - y, x, c)

    loads = [pltpu.make_async_copy(src, dst, ld_sem.at[i]) for i, (src, dst) in enumerate((
        (k_hbm, kb.at[own]), (v_hbm, vb.at[own]), (q_hbm, qb.at[y]), (do_hbm, dob.at[y]), (o_hbm, ob), (lse_hbm, lseb)))]
    for load in loads:
        load.start()

    barrier = pltpu.get_barrier_semaphore()
    peers = [partner] + [dev(y, wrap(x + d), c) for d in (1, 3)] + [dev(wrap(y + d), x, c) for d in (1, 3)]
    for peer in peers:
        pl.semaphore_signal(barrier, inc=1, device_id={'cp': peer}, device_id_type=MESH)
    pl.semaphore_wait(barrier, len(peers))

    def kv_pair(slot, ssem, device):
        return (copy(kb.at[slot], kb.at[slot], ssem.at[0], kv_rs.at[slot, 0], device),
                copy(vb.at[slot], vb.at[slot], ssem.at[1], kv_rs.at[slot, 1], device))

    def start(pair):
        for p in pair:
            p.start()

    def kv_wait(slot):
        for p in kv_pair(slot, kv_s3, partner):
            p.wait_recv()

    def q_trio(row, dst_row, relayed=0, parts=(0, 1, 2)):
        device = dev(dst_row, x, c)
        return tuple(copy(b.at[row], b.at[row], q_ss.at[4 * relayed + dst_row, i], q_rs.at[row, i], device)
                     for i, b in enumerate((qb, dob, stb)) if i in parts)

    def q_wait(row, parts=(0, 1, 2)):
        for p in q_trio(row, row, 0, parts):
            p.wait_recv()

    def kv_onward(slot, taken, toward):
        buf = kb if toward == 0 else vb
        return copy(buf.at[slot], buf.at[slot], kv_s5.at[2 * taken + toward], kv_rs.at[slot, toward],
                    dev(y, wrap(x + (1 if toward == 0 else 3)), c))

    def par_copy(slot, idx):
        return copy(dkv.at[slot], par.at[idx], par_ss.at[idx], par_rs.at[idx], partner)

    def ici_copy(slot, cls, side_in, h):
        device = dev(y, jnp.where(side_in == 0, wrap(x + 1), wrap(x + 3)), c)
        return copy(dkv.at[slot, h], ici.at[2 * cls + side_in, h], ici_ss.at[2 * cls + side_in, h],
                    ici_rs.at[2 * cls + side_in, h], device)

    def half_copy(slot, cls, h):
        return copy(dkv.at[slot, h], half.at[2 * cls + h], half_ss.at[2 * cls + h], half_rs.at[2 * cls + h],
                    dev(y, wrap(x + (1 if h == 0 else 3)), c))

    def dq_copy(row, h):
        up = row == y + 1
        dst = jnp.where(y == 3, jnp.where(row == 1, 0, 2), jnp.where(row == y + 3, 3, y + 1))
        place = jnp.where(up, 1, jnp.where(jnp.logical_or(row == y + 3, row == y - 1), 2, 0))
        part = pl.ds(h * tok, tok)
        return copy(dqa.at[row, part], dqr.at[place, part], dq_ss.at[row, h], dq_rs.at[place, h], dev(dst, x, c))

    def dq_take(row, place, h):
        half_rows = pl.ds(h * tok, tok)
        copy(dqa.at[row, half_rows], dqr.at[place, half_rows], dq_ss.at[0, h], dq_rs.at[place, h], partner).wait_recv()

        def body(i, carry):
            part = pl.ds(pl.multiple_of(h * tok + i * sub, sub), sub)
            dqa[row, part, :] += dqr[place, part, :]
            return carry
        lax.fori_loop(0, tok // sub, body, 0)

    def fin_copy(h):
        return copy(dkv.at[8 + x, h], fin.at[h], fin_ss.at[h], fin_rs.at[h], mirror)

    for load in loads[:2]:
        load.wait()
    start(kv_pair(own, kv_s1.at[0], partner))
    for d in (1, 3):
        start(kv_pair(own, kv_s1.at[d], dev(y, wrap(x + d), c)))

    def give_copy():
        slot = 8 + x
        return (copy(kb.at[own], kb.at[slot], kv_s3.at[0], kv_rs.at[slot, 0], mirror),
                copy(vb.at[own], vb.at[slot], kv_s3.at[1], kv_rs.at[slot, 1], mirror))

    @pl.when(gives)
    def _():
        start(give_copy())

    for load in loads[2:]:
        load.wait()

    def feed(parts):
        for d in (1, 3):
            dst = wrap(y + d)

            @pl.when(feeds(dst, y))
            def _():
                start(q_trio(y, dst, 0, parts))

    feed((0, 1))

    def clear(ref, slots):
        def body(i, carry):
            ref[i] = jnp.zeros(ref.shape[1:], F32)
            return carry
        lax.fori_loop(0, slots, body, 0)

    def row_stats():
        stb[y] = jnp.zeros(stb.shape[1:], F32)
        pair = (sub // 2, sub)
        spread = (lax.broadcasted_iota(jnp.int32, pair, 1) // 2 == lax.broadcasted_iota(jnp.int32, pair, 0)).astype(F32)
        even = lax.broadcasted_iota(jnp.int32, (1, sub), 1) % 2 == 0
        for p in range(rows2 // sub):
            part = pl.ds(p * sub, sub)
            lse = lseb[:, pl.ds(p * sub // 2, sub // 2)] * math.log2(math.e)
            lse = jnp.dot(lse, spread, precision=lax.Precision.HIGHEST, preferred_element_type=F32)
            stb[y, 0:1, part] = jnp.where(even, lse[0:1], lse[1:2])
            prod = dob[y, part, :].astype(F32) * ob[part, :].astype(F32)
            stb[y, 1:2, part] = jnp.sum(prod.T, axis=0, keepdims=True)

    row_stats()
    clear(dkv, dkv.shape[0])
    feed((2,))
    clear(dqa, dqa.shape[0])

    def transpose_queries(row):
        for g in range(8):
            part = pl.ds(g * sub, sub)
            qtb[row, :, part] = qb[row, part, :].T
            dotb[row, :, part] = dob[row, part, :].T

    def piece(row, slot, start_row, width, u, masked):
        part = pl.ds(start_row, sub)
        k_t = kb[slot, :width, :]
        logits = lax.dot_general(qb[row, part, :], k_t, NT, preferred_element_type=F32)
        d_prob = lax.dot_general(dob[row, part, :], vb[slot, :width, :], NT, preferred_element_type=F32)
        stats = stb[row, :, part].T
        power = logits * exp_scale - stats[:, 0:1]
        if masked:
            r = (lax.broadcasted_iota(jnp.int32, power.shape, 0) + u * sub) // 2
            power = jnp.where(lax.broadcasted_iota(jnp.int32, power.shape, 1) <= r, power, -1e30)
        prob = jnp.exp2(power)
        d_score = (prob * (d_prob - stats[:, 1:2])).astype(BF16)
        prob = prob.astype(BF16)
        dkv[slot, 1, :, :width] += jnp.dot(dotb[row, :, part], prob, preferred_element_type=F32)
        dkv[slot, 0, :, :width] += jnp.dot(qtb[row, :, part], d_score, preferred_element_type=F32)
        dqa[row, part, :] += jnp.dot(d_score, k_t, preferred_element_type=F32)

    def full_task(row, slot, first_half, end_half):
        def half_loop(g, carry):
            for u in range(tok // sub):
                piece(row, slot, pl.multiple_of(g * tok + u * sub, sub), tok, 0, False)
            return carry
        lax.fori_loop(first_half, end_half, half_loop, 0)

    def diag_task():
        for u in range(8):
            piece(y, own, u * sub, (u // 2 + 1) * sub, u, True)

    def add_into(slot, h, other):
        def body(i, carry):
            part = pl.ds(pl.multiple_of(i * 32, 32), 32)
            dkv[slot, h, part, :] += other[part, :]
            return carry
        lax.fori_loop(0, head // 32, body, 0)

    def meets(xx, xs, cc):
        return jnp.logical_or(jnp.logical_not(local_only(y, xs, cc)), xx >= xs)

    def sum_chip(slot, xs, idx, cls):
        par_copy(slot, idx).wait_recv()
        for h in range(2):
            add_into(slot, h, par.at[idx, h])

        @pl.when(xs == wrap(x + 2))
        def _():
            for h in range(2):
                half_copy(slot, cls, h).start()

    def pass_on(slot, xs, cls, joined):
        for h in range(2):
            @pl.when(xs == wrap(x + (1 if h == 0 else 3)))
            def _():
                @pl.when(joined)
                def _():
                    half_copy(slot, cls, h).wait_recv()
                    add_into(slot, h, half.at[2 * cls + h])
                for part in range(2):
                    ici_copy(slot, cls, h, part).start()

    transpose_queries(y)
    diag_task()

    @pl.when(takes)
    def _():
        kv_wait(8 + x)
        start(kv_pair(8 + x, kv_s4.at[0], partner))
        for d in (1, 3):
            start(kv_pair(8 + x, kv_s4.at[d], dev(y, wrap(x + d), c)))

    def after_diag(stage):
        for xs in range(4):
            cc = 1 - c if stage == 0 else c
            alone = local_only(y, xs, cc)

            @pl.when(jnp.logical_and(alone, xs <= x if stage < 2 else jnp.logical_or(xs <= x, (xs + 2) % 4 >= xs)))
            def _():
                if stage == 0:
                    par_copy(2 * xs + 1 - c, xs).start()
                elif stage == 1:
                    sum_chip(2 * xs + c, xs, xs, 0)
                else:
                    pass_on(2 * xs + c, xs, 0, (xs + 2) % 4 >= xs)

    def taken_at(xs):
        return jnp.logical_or(y == 3, jnp.logical_and(y == 2, xs < 2))

    def step(t, carry):
        half = t // 2
        d = half + jnp.where(half == 2, 1, 0) - jnp.where(half == 3, 1, 0)
        x_d = wrap(x + d)
        mate = lax.rem(t, 2)
        c_d = jnp.where(mate == 0, c, 1 - c)
        v = jnp.maximum(t - 8, 0)
        u, part, ends = unit(v)
        whole = v < WHOLE
        first = t < 8
        slot_u, xs, idx, resp = decode(u)
        slot = jnp.where(first, 2 * x_d + c_d, slot_u)
        row = jnp.where(first, y, field(T_Q, 2, u))

        later = jnp.logical_not(first)
        fresh = jnp.logical_and(later, whole)

        @pl.when(jnp.logical_and(first, mate == 1))
        def _():
            kv_wait(slot)

        @pl.when(t == 2)
        def _():
            for toward, dd in ((0, 3), (1, 1)):
                near = 2 * wrap(x + dd) + c
                kv_wait(near)
                kv_onward(near, 0, toward).start()
                start(kv_pair(near, kv_s2.at[wrap(x + dd)], partner))

        @pl.when(t == 6)
        def _():
            kv_wait(slot)
            start(kv_pair(slot, kv_s2.at[x_d], partner))

        for when, parts in ((3, (0,)), (5, (1, 2))):
            @pl.when(jnp.logical_and(t == when, y == 0))
            def _():
                q_wait(3, parts)
                start(q_trio(3, 1, 1, parts))
                q_wait(1, parts)
                start(q_trio(1, 3, 1, parts))

            @pl.when(jnp.logical_and(t == when, y == 1))
            def _():
                q_wait(2, parts)
                start(q_trio(2, 0, 1, parts))

        @pl.when(jnp.logical_and(t == 7, c == 0))
        def _():
            for toward, dd in ((0, 3), (1, 1)):
                near = wrap(x + dd)

                @pl.when(taken_at(near))
                def _():
                    kv_wait(8 + near)
                    kv_onward(8 + near, 1, toward).start()
                    start(kv_pair(8 + near, kv_s2.at[4 + near], partner))

        @pl.when(jnp.logical_and(fresh, field(T_QFIRST, 1, u) == 1))
        def _():
            relayed = jnp.logical_or(jnp.logical_and(y == 0, row != 2), jnp.logical_and(y == 1, row == 2))

            @pl.when(jnp.logical_not(relayed))
            def _():
                q_wait(row)
            transpose_queries(row)

        @pl.when(jnp.logical_and(fresh, field(T_TAKEN, 1, u) == 1))
        def _():
            far = xs == wrap(x + 2)

            @pl.when(jnp.logical_or(c == 1, far))
            def _():
                kv_wait(slot)

            @pl.when(jnp.logical_and(c == 0, far))
            def _():
                start(kv_pair(slot, kv_s2.at[4 + xs], partner))

        @pl.when(jnp.logical_or(later, 2 * x_d + c_d < own))
        def _():
            full_task(row, slot, jnp.where(whole, 0, part), jnp.where(whole, 2, part + 1))

        for stage, when in ((0, 12), (1, 14), (2, 16)):
            @pl.when(t == when)
            def _():
                after_diag(stage)

        for h in range(2):
            @pl.when(jnp.logical_and(jnp.logical_and(later, field(T_QLAST, 1, u) == 1), jnp.logical_or(whole, part == h)))
            def _():
                @pl.when(row == y + 1)
                def _():
                    dq_take(row, 0, h)
                dq_copy(row, h).start()

        done = jnp.logical_and(ends, field(T_KVLAST, 1, u) == 1)

        @pl.when(jnp.logical_and(later, jnp.logical_and(done, c != resp)))
        def _():
            par_copy(slot, idx).start()

        def finished(back, action):
            before, _, ends_b = unit(jnp.maximum(v - back, 0))
            slot_b, xs_b, idx_b, resp_b = decode(before)
            ready = jnp.logical_and(ends_b, field(T_KVLAST, 1, before) == 1)

            @pl.when(jnp.logical_and(v >= back, jnp.logical_and(ready, c == resp_b)))
            def _():
                action(slot_b, xs_b, idx_b)

        finished(1, lambda slot_b, xs_b, idx_b: sum_chip(slot_b, xs_b, idx_b, idx_b // 4))
        finished(1 + DELAY, lambda slot_b, xs_b, idx_b: pass_on(slot_b, xs_b, idx_b // 4, True))
        return carry

    lax.fori_loop(1, 8 + N_STEP, step, 0)

    for v_b in range(N_STEP - 1 - DELAY, N_STEP):
        u_b, _, ends_b = unit(jnp.int32(v_b))
        slot_b, xs_b, idx_b, resp_b = decode(u_b)

        @pl.when(jnp.logical_and(jnp.logical_and(ends_b, field(T_KVLAST, 1, u_b) == 1), c == resp_b))
        def _():
            if v_b == N_STEP - 1:
                sum_chip(slot_b, xs_b, idx_b, idx_b // 4)
            pass_on(slot_b, xs_b, idx_b // 4, True)

    def from_side(slot, cls, side_in, h):
        ici_copy(slot, cls, side_in, h).wait_recv()
        add_into(slot, h, ici.at[2 * cls + side_in, h])

    @pl.when(takes)
    def _():
        for h in range(2):
            for side_in in range(2):
                from_side(8 + x, 1, side_in, h)
            fin_copy(h).start()

    for side_in in range(2):
        near = wrap(x + (3 if side_in == 0 else 1))

        @pl.when(jnp.logical_or(meets(near, x, c), meets(wrap(x + 2), x, c)))
        def _():
            for h in range(2):
                from_side(own, 0, side_in, h)

    for h in range(2):
        @pl.when(y >= 1)
        def _():
            dq_take(y, 1, h)

        @pl.when(y >= 2)
        def _():
            dq_take(y, 2, h)

    @pl.when(gives)
    def _():
        for h in range(2):
            fin_copy(h).wait_recv()
            add_into(own, h, fin.at[h])

    def out_q(i, carry):
        part = pl.ds(pl.multiple_of(i * sub, sub), sub)
        gq_ref[part, :] = (dqa[y, part, :] * scale).astype(BF16)
        return carry

    lax.fori_loop(0, rows2 // sub, out_q, 0)
    for g in range(4):
        part = pl.ds(g * sub, sub)
        gk_ref[part, :] = (dkv[own, 0, :, part] * scale).T.astype(BF16)
        gv_ref[part, :] = dkv[own, 1, :, part].T.astype(BF16)

    def sent(pair):
        for p in pair:
            p.wait_send()

    for d in (0, 1, 3):
        sent(kv_pair(own, kv_s1.at[d], partner))
    for h in range(2):
        kv_onward(own, 0, h).wait_send()
    for d in (1, 2, 3):
        sent(kv_pair(own, kv_s2.at[wrap(x + d)], partner))
    for d in (1, 3):
        dst = wrap(y + d)

        @pl.when(feeds(dst, y))
        def _():
            sent(q_trio(y, dst))

    @pl.when(y == 0)
    def _():
        sent(q_trio(3, 1, 1))
        sent(q_trio(1, 3, 1))

    @pl.when(y == 1)
    def _():
        sent(q_trio(2, 0, 1))

    for row in (1, 2, 3):
        @pl.when(jnp.logical_and(row != y, feeds(y, row)))
        def _():
            for h in range(2):
                dq_copy(row, h).wait_send()

    @pl.when(gives)
    def _():
        sent(give_copy())

    @pl.when(takes)
    def _():
        for d in (0, 1, 3):
            sent(kv_pair(8 + x, kv_s4.at[d], partner))
        for h in range(2):
            fin_copy(h).wait_send()

    for xs in range(4):
        @pl.when(meets(x, xs, 1 - c))
        def _():
            par_copy(2 * xs + 1 - c, xs).wait_send()

        @pl.when(jnp.logical_and(c == 1, taken_at(xs)))
        def _():
            par_copy(8 + xs, 4 + xs).wait_send()

        @pl.when(jnp.logical_and(jnp.logical_and(c == 0, xs != x), taken_at(xs)))
        def _():
            sent(kv_pair(8 + xs, kv_s2.at[4 + xs], partner))

    far = wrap(x + 2)
    for h in range(2):
        behind = wrap(x + (3 if h == 0 else 1))
        ahead = wrap(x + (1 if h == 0 else 3))

        @pl.when(jnp.logical_and(c == 0, taken_at(behind)))
        def _():
            kv_onward(8 + x, 1, h).wait_send()

        @pl.when(meets(x, far, c))
        def _():
            half_copy(own, 0, h).wait_send()

        @pl.when(jnp.logical_or(meets(x, ahead, c), meets(behind, ahead, c)))
        def _():
            for part in range(2):
                ici_copy(own, 0, h, part).wait_send()

        @pl.when(jnp.logical_and(c == 0, taken_at(far)))
        def _():
            half_copy(own, 1, h).wait_send()

        @pl.when(jnp.logical_and(c == 0, taken_at(ahead)))
        def _():
            for part in range(2):
                ici_copy(own, 1, h, part).wait_send()


def solution(mesh):
    n_dev = mesh.shape['cp']
    side = math.isqrt(n_dev // 2)
    assert side * side * 2 == n_dev and side == len(ROWS)
    row_spec = P(('dp', 'cp'))

    def local_fn(q_tok, k_tok, v_tok, fwd_out, d_out, lse_row):
        tok, heads, head = q_tok.shape
        scale = head ** -0.5
        rows2 = tok * heads
        q_rows = q_tok.reshape(rows2, head)
        do_rows = d_out.reshape(rows2, head)
        o_rows = fwd_out.reshape(rows2, head)
        hbm = pl.BlockSpec(memory_space=pl.ANY)
        vmem = pl.BlockSpec(memory_space=pltpu.VMEM)
        slots = 3 * side
        line, grid = pltpu.SemaphoreType.DMA((8,)), pltpu.SemaphoreType.DMA((slots, 3))
        rows_low = pltpu.VMEM((side, rows2, head), BF16)
        cols_low = pltpu.VMEM((side, head, rows2), BF16)
        keys = pltpu.VMEM((slots, tok, head), BF16)

        def sums(n):
            return pltpu.VMEM((n, 2, head, tok), F32)

        gq, gk, gv = pl.pallas_call(
            functools.partial(attn_grad_kernel, side, scale),
            out_shape=[jax.ShapeDtypeStruct((rows2, head), BF16), jax.ShapeDtypeStruct((tok, head), BF16),
                       jax.ShapeDtypeStruct((tok, head), BF16)],
            in_specs=[hbm] * 6,
            out_specs=[vmem] * 3,
            scratch_shapes=[
                rows_low, rows_low, pltpu.VMEM((side, 8, rows2), F32), pltpu.VMEM((rows2, head), BF16),
                pltpu.VMEM((heads, tok), F32), cols_low, cols_low, keys, keys, pltpu.VMEM((side, rows2, head), F32),
                sums(slots), pltpu.VMEM((3, rows2, head), F32), sums(8), sums(side), pltpu.VMEM((side, head, tok), F32),
                pltpu.VMEM((2, head, tok), F32), line, grid, grid, grid, grid, line, grid, line, grid,
                line, line, grid, grid, line, line, grid, grid, line, line,
            ],
            compiler_params=pltpu.CompilerParams(collective_id=0, has_side_effects=True, vmem_limit_bytes=66 * 10 ** 6),
            name='attn_grad',
        )(q_rows, do_rows, o_rows, lse_row.T, k_tok, v_tok)
        return gq.reshape(tok, heads, head), gk, gv

    return jax.shard_map(local_fn, mesh=mesh, in_specs=(row_spec,) * 6, out_specs=(row_spec,) * 3, check_vma=False)
```
